256 devices in a mesh: sx: 4 (over z_hi), sy: 4 (over x), fq: 16 (over y, z_lo, core).
Axes of the slice: x: 4, y: 4, z: 8 (z_hi: 4, z_lo: 2; z = z_hi * 2 + z_lo), core: 2. Of those that a mesh axis runs over, the one named last changes fastest.
Arguments:
- spectra: bfloat16 [128, 2, 128, 64, 512], P('fq', None, 'sx', 'sy'), may hold values from -0.125 to 0.125
- noise_weight: float32 [512, 256], P(('sx', 'sy')), may hold values from 0.5 to 2
- class_map: int32 [128, 64], P('sx', 'sy'), may hold values from 0 to 7
- class_kappa: float32 [8], replicated, may hold values from 0.25 to 4
- solution: float32 [128, 512, 256], P('fq', ('sx', 'sy')), may hold values from -6 to 6
- residual: float32 [128, 512, 256], P('fq', ('sx', 'sy')), may hold values from -6 to 6
- direction: float32 [128, 512, 256], P('fq', ('sx', 'sy')), may hold values from -6 to 6
- step_length: float32 [128], P('fq'), may hold values from 0.2 to 1
- old_norm: float32 [128], P('fq'), may hold values from 131072 to 524288
Outputs:
- new_solution: float32 [128, 512, 256], P('fq', ('sx', 'sy'))
- new_residual: float32 [128, 512, 256], P('fq', ('sx', 'sy'))
- new_direction: float32 [128, 512, 256], P('fq', ('sx', 'sy'))
- new_norm: float32 [128], P('fq')
The draws below stay inside these ranges and needn't reach their ends.
All inputs are finite; a program needn't handle non-finite values.
Results may differ from the reference program's by a relative error of at most 0.0022.
Values may be sent and summed in bfloat16 or wider, within the bound.
A program may use at most 128 MiB of HBM per device.

```python
import math
import jax
import jax.numpy as jnp
from jax import lax

SENS = 512
SWEEPS = 4
NCLS = 8
NX = 128
NY = 64
FREQ = 128
NT = 256
COLS = 128


def set_ends(array, rng, low, top_value):
    extent = array.shape
    index_at = [jax.random.randint(jax.random.fold_in(rng, axis), (), 0, extent[axis]) for axis in range(len(extent))]
    array = array.at[tuple(index_at)].set(low)
    longest = extent.index(max(extent))
    index_at[longest] = (index_at[longest] + 1) % extent[longest]
    return array.at[tuple(index_at)].set(top_value)


def block_levels(stream_key, shape, shards, low, high):
    gain = 1.0
    for dim, shards_of in shards:
        steps = jax.random.uniform(jax.random.fold_in(jax.random.fold_in(stream_key, 6), dim), (shards_of,), jnp.float32, low / len(shards), high / len(shards))
        gain = gain * jnp.repeat(jnp.exp(steps), shape[dim] // shards_of).reshape((-1,) + (1,) * (len(shape) - 1 - dim))
    return gain


def bell_draw(own_key, shape, width, most, pieces=(), kind=jnp.bfloat16):
    entries = jax.random.normal(own_key, shape, jnp.float32) * width
    if len(pieces) > 0:
        entries = block_levels(own_key, shape, pieces, -0.22, 0.18) * entries
    return jnp.clip(entries, min=-most, max=most).astype(kind)


def setup_inputs(seed: int = 0) -> dict:
    seeds = jax.random.split(jax.random.key(seed), 10)
    spectra = bell_draw(seeds[0], (FREQ, 2, NX, NY, SENS), (4 * SENS) ** -0.5, 0.125, ((0, 16), (2, 4), (3, 4)))
    noise_weight = jnp.clip(jnp.exp(math.log(2.0) - 1.3862944 * jax.random.uniform(seeds[1], (SENS, NT), jnp.float32) ** block_levels(seeds[1], (SENS, NT), ((0, 16),), -0.2, 0.2)), 0.5, 2.0)
    class_map = set_ends(jax.random.randint(seeds[2], (NX, NY), 0, NCLS), jax.random.fold_in(seeds[2], 1), 0, NCLS - 1).astype(jnp.int32)
    class_kappa = jnp.clip(jnp.exp(jax.random.uniform(seeds[3], (NCLS,), jnp.float32, math.log(0.25), math.log(4.0))), 0.25, 4.0)
    solution = bell_draw(seeds[4], (COLS, SENS, NT), 1.0, 6.0, ((0, 16), (1, 16)), jnp.float32)
    residual = bell_draw(seeds[5], (COLS, SENS, NT), 1.0, 6.0, ((0, 16), (1, 16)), jnp.float32)
    direction = bell_draw(seeds[6], (COLS, SENS, NT), 1.0, 6.0, ((0, 16), (1, 16)), jnp.float32)
    step_length = jnp.clip(jnp.exp(math.log(1.0) - 1.609438 * jax.random.uniform(seeds[7], (COLS,), jnp.float32) ** block_levels(seeds[7], (COLS,), ((0, 16),), -0.2, 0.2)), 0.2, 1.0)
    old_norm = jnp.clip(jnp.exp(math.log(524288.0) - 1.3862944 * jax.random.uniform(seeds[8], (COLS,), jnp.float32) ** block_levels(seeds[8], (COLS,), ((0, 16),), -0.2, 0.2)), 131072.0, 524288.0)
    return {"spectra": spectra, "noise_weight": noise_weight, "class_map": class_map, "class_kappa": class_kappa, "solution": solution, "residual": residual, "direction": direction, "step_length": step_length, "old_norm": old_norm}


HIGHEST = lax.Precision.HIGHEST

def tables(freq_count, time_steps):
    freq_index = jnp.arange(freq_count, dtype=jnp.int32)[:, None]
    step_index = jnp.arange(time_steps, dtype=jnp.int32)[None, :]
    phases = (freq_index * step_index % time_steps).astype(jnp.float32) * (2.0 * math.pi / time_steps)
    factor = 1.0 / math.sqrt(time_steps)
    cosine_table = jnp.cos(phases) * factor
    sine_table = jnp.sin(phases) * factor
    doubling = jnp.where(jnp.arange(freq_count, dtype=jnp.int32) == 0, 1.0, 2.0).astype(jnp.float32)
    return (cosine_table, sine_table, doubling)

def neighbours(padded):
    return padded[2:, 1:-1] + padded[:-2, 1:-1] + padded[1:-1, 2:] + padded[1:-1, :-2]

def reference(spectra, noise_weight, class_map, class_kappa, solution, residual, direction, step_length, old_norm):
    cosine_table, sine_table, doubling = tables(FREQ, NT)
    weighted = noise_weight[None] * direction
    spec_real = jnp.einsum('kst,ft->fks', weighted, cosine_table, precision=HIGHEST).astype(jnp.bfloat16)
    spec_imag = (-jnp.einsum('kst,ft->fks', weighted, sine_table, precision=HIGHEST)).astype(jnp.bfloat16)
    kappa_cells = class_kappa[class_map][:, :, None]
    denom = 1.0 + 4.0 * kappa_cells

    def one_freq(inputs):
        weights, query_real, query_imag = inputs
        real_part = weights[0].astype(jnp.float32)
        imag_part = weights[1].astype(jnp.float32)
        query_real = query_real.astype(jnp.float32)
        query_imag = query_imag.astype(jnp.float32)
        pattern = 'xys,ks->xyk'
        adjoint_real = jnp.einsum(pattern, real_part, query_real) + jnp.einsum(pattern, imag_part, query_imag)
        adjoint_imag = jnp.einsum(pattern, real_part, query_imag) - jnp.einsum(pattern, imag_part, query_real)
        source = jnp.concatenate([adjoint_real, adjoint_imag], axis=2)
        smooth = source / denom
        for sweep_index in range(SWEEPS - 1):
            padded = jnp.pad(smooth, ((1, 1), (1, 1), (0, 0)))
            smooth = (source + kappa_cells * neighbours(padded)) / denom
        field_half = lax.optimization_barrier(smooth.astype(jnp.bfloat16))
        field_full = field_half.astype(jnp.float32)
        field_real = field_full[:, :, :COLS]
        field_imag = field_full[:, :, COLS:]
        forward = 'xys,xyk->sk'
        out_real = jnp.einsum(forward, real_part, field_real) - jnp.einsum(forward, imag_part, field_imag)
        out_imag = jnp.einsum(forward, real_part, field_imag) + jnp.einsum(forward, imag_part, field_real)
        return (out_real, out_imag)
    sums_real, sums_imag = lax.map(one_freq, (spectra, spec_real, spec_imag))
    scaled_real = sums_real * doubling[:, None, None]
    scaled_imag = sums_imag * doubling[:, None, None]
    returned = jnp.einsum('fsk,ft->kst', scaled_real, cosine_table, precision=HIGHEST) - jnp.einsum('fsk,ft->kst', scaled_imag, sine_table, precision=HIGHEST)
    product = direction + noise_weight[None] * returned
    new_solution = solution + step_length[:, None, None] * direction
    new_residual = residual - step_length[:, None, None] * product
    new_norm = lax.optimization_barrier(jnp.sum(new_residual * new_residual, axis=(1, 2)))
    new_direction = new_residual + (new_norm / old_norm)[:, None, None] * direction
    return (new_solution, new_residual, new_direction, new_norm)
```

```python
import functools
import math

import jax
import jax.numpy as jnp
import numpy as np
from jax import lax
from jax.experimental import pallas as pl
from jax.experimental.pallas import tpu as pltpu
from jax.sharding import PartitionSpec as P

MESH = pl.DeviceIdType.MESH
HIGHEST = lax.Precision.HIGHEST
BF, F32 = jnp.bfloat16, jnp.float32
PITCH = 24
NF = 8
G = 4


def tables(freq_count, time_steps, per_block):
    freq = np.arange(freq_count)
    phase = (freq[:, None] * np.arange(time_steps)[None, :] % time_steps) * (2.0 * math.pi / time_steps)
    factor = 1.0 / math.sqrt(time_steps)
    both = np.stack([np.cos(phase), -np.sin(phase)], axis=1) * factor
    doubled = both * np.where(freq == 0, 1.0, 2.0)[:, None, None]
    forward = both.reshape(2 * freq_count, time_steps).T
    back = doubled.reshape(2 * freq_count, time_steps)
    return forward.astype(np.float32), back.astype(np.float32)


def swapped(arrays, unit):
    arrays = list(arrays)
    lane = lax.broadcasted_iota(jnp.int32, arrays[0].shape, 1)
    bit = 1
    while bit < len(arrays):
        here = ((lane // unit) & bit) != 0
        for i in range(len(arrays)):
            if i & bit == 0:
                a, c = arrays[i], arrays[i | bit]
                arrays[i] = jnp.where(here, pltpu.roll(c, bit * unit, 1), a)
                arrays[i | bit] = jnp.where(here, c, pltpu.roll(a, 128 - bit * unit, 1))
        bit *= 2
    return arrays


def remote(src, dst, send, recv, device):
    return pltpu.make_async_remote_copy(
        src_ref=src, dst_ref=dst, send_sem=send, recv_sem=recv, device_id=device, device_id_type=MESH
    )


def kernel(
    dir_ref, res_ref, noise_ref, map_ref, kap_ref, step_ref, fwd_ref, back_ref, spectra_ref,
    new_res_ref, norm_ref,
    a, at, q, b0, p1, p2, kd, inv, out, sx_buf, fin, a2s, a2r, r2s, r2r,
    hxs, hxr, hys, hyr, rxf, rxd, rxc, rzf, rzd, rzc, ns, nr, fh,
    a_sem, as_sem, ar_sem, bs_sem, br_sem, ns_sem, nr_sem,
    zs, zr, xs, xr, hs, hr, rxs, rxr, rzs, rzr,
):
    sx, sy, fq = lax.axis_index("sx"), lax.axis_index("sy"), lax.axis_index("fq")
    tile = sx * G + sy

    def add(i, d, n):
        return lax.rem(i + d + n, n)

    def on_z(d):
        return (add(sx, d, G), sy, fq)

    def on_x(d):
        return (sx, add(sy, d, G), fq)

    def in_fq(d):
        return (sx, sy, add(fq, d, 16))

    def in_tiles(d):
        other = add(tile, d, 16)
        return (other // G, lax.rem(other, G), fq)

    barrier = pltpu.get_barrier_semaphore()
    for d in range(1, 16):
        pl.semaphore_signal(barrier, inc=1, device_id=in_fq(d), device_id_type=MESH)
        pl.semaphore_signal(barrier, inc=1, device_id=in_tiles(d), device_id_type=MESH)

    def a_copy(f):
        return pltpu.make_async_copy(spectra_ref.at[f], a.at[f], a_sem.at[f])

    for f in range(NF):
        a_copy(f).start()

    weighted = (dir_ref[...] * noise_ref[...][None]).reshape(256, 256)
    spec = jnp.dot(weighted, fwd_ref[...], preferred_element_type=F32, precision=HIGHEST)
    for half in range(2):
        part = [spec[32 * k : 32 * k + 32, 128 * half : 128 * half + 128] for k in range(8)]
        for i, chunk in enumerate(swapped(part, 16)):
            a2s[8 * half + i] = chunk.astype(BF)
    pl.semaphore_wait(barrier, 30)

    def a_exchange(d, src, dst, ss, rs):
        peer = in_fq(d)
        return remote(src.at[peer[2]], dst.at[fq], ss.at[d], rs.at[d], peer)

    def a_arrival(d, dst, ss, rs):
        peer = in_fq(-d)
        return remote(dst.at[peer[2]], dst.at[peer[2]], ss.at[d], rs.at[d], peer)

    for d in range(1, 16):
        a_exchange(d, a2s, a2r, as_sem, ar_sem).start()
    a2r[fq] = a2s[fq]

    classes = map_ref[...]
    kappa = jnp.zeros(classes.shape, F32)
    for c in range(8):
        kappa = jnp.where(classes == c, kap_ref[c], kappa)
    eye = lax.broadcasted_iota(jnp.int32, (16, 16), 0) == lax.broadcasted_iota(jnp.int32, (16, 16), 1)
    for x in range(32):
        row = jnp.broadcast_to(kappa[x : x + 1, :], (16, 16))
        column = jnp.sum(jnp.where(eye, row, 0.0), axis=1, keepdims=True)
        scale = 1.0 / (1.0 + 4.0 * column)
        inv[x] = jnp.broadcast_to(scale, (16, 128))
        kd[x] = jnp.broadcast_to(scale * column, (16, 128))

    zero_x = jnp.zeros((NF, 2, 16, 128), F32)
    zero_y = jnp.zeros((32, 128), F32)
    low_x, high_x = pl.ds(0, 16), pl.ds(33 * PITCH, 16)
    low_y, high_y = pl.ds(PITCH - 1, 32, stride=PITCH), pl.ds(PITCH + 16, 32, stride=PITCH)
    padded = (b0, p1, p2)

    @pl.when(sx == 0)
    def _():
        for p in padded:
            p[:, :, low_x, :] = zero_x

    @pl.when(sx == G - 1)
    def _():
        for p in padded:
            p[:, :, high_x, :] = zero_x

    @pl.when(sy == 0)
    def _():
        @pl.loop(0, NF)
        def _(f):
            for p in padded:
                for c in range(2):
                    p[f, c, low_y, :] = zero_y

    @pl.when(sy == G - 1)
    def _():
        @pl.loop(0, NF)
        def _(f):
            for p in padded:
                for c in range(2):
                    p[f, c, high_y, :] = zero_y

    for f in range(NF):
        a_copy(f).wait()
    for d in range(1, 16):
        a_arrival(d, a2r, as_sem, ar_sem).wait_recv()
    for i, block in enumerate(swapped([a2r[kb].astype(F32) for kb in range(16)], 1)):
        q[i // 2, sx, sy, i % 2] = block.astype(BF)

    def z_own(f, side):
        return remote(q.at[f, sx, sy], q.at[f, sx, sy], zs.at[f, side], zr.at[f, side], on_z(1 - 2 * side))

    def z_relay(f):
        side = lax.rem(f, 2)
        block = q.at[f, add(sx, 3 + 2 * side, G), sy]
        return remote(block, block, zs.at[f, 2], zr.at[f, 2], on_z(1 + 2 * side))

    def z_in(f, side):
        block = q.at[f, add(sx, 3 + 2 * side, G), sy]
        return remote(block, block, zs.at[f, side], zr.at[f, side], on_z(1))

    def z_far(f):
        block = q.at[f, add(sx, 2, G), sy]
        return remote(block, block, zs.at[f, 2], zr.at[f, 2], on_z(1))

    def x_own(f, side):
        block = q.at[f, :, sy]
        return remote(block, block, xs.at[f, side], xr.at[f, side], on_x(1 - 2 * side))

    def x_relay(f):
        side = lax.rem(f, 2)
        block = q.at[f, :, add(sy, 3 + 2 * side, G)]
        return remote(block, block, xs.at[f, 2], xr.at[f, 2], on_x(1 + 2 * side))

    def x_in(f, side):
        block = q.at[f, :, add(sy, 3 + 2 * side, G)]
        return remote(block, block, xs.at[f, side], xr.at[f, side], on_x(1))

    def x_far(f):
        block = q.at[f, :, add(sy, 2, G)]
        return remote(block, block, xs.at[f, 2], xr.at[f, 2], on_x(1))

    sides = ((sx > 0, on_z(-1)), (sx < G - 1, on_z(1)), (sy > 0, on_x(-1)), (sy < G - 1, on_x(1)))

    def h_out(j, f, side):
        s, r = (hxs, hxr) if side < 2 else (hys, hyr)
        return remote(
            s.at[j, f, side % 2], r.at[j, f, 1 - side % 2],
            hs.at[j, f, side], hr.at[j, f, side ^ 1], sides[side][1],
        )

    def h_in(j, f, side):
        r = hxr if side < 2 else hyr
        return remote(
            r.at[j, f, side % 2], r.at[j, f, side % 2], hs.at[j, f, side], hr.at[j, f, side], sides[side][1]
        )

    def send_edges(j, f, p):
        for c in range(2):
            hxs[j, f, 0, c] = p[f, c, pl.ds(PITCH, 16), :].astype(BF)
            hxs[j, f, 1, c] = p[f, c, pl.ds(32 * PITCH, 16), :].astype(BF)
            hys[j, f, 0, c] = p[f, c, pl.ds(PITCH, 32, stride=PITCH), :].astype(BF)
            hys[j, f, 1, c] = p[f, c, pl.ds(PITCH + 15, 32, stride=PITCH), :].astype(BF)
        for side in range(4):
            @pl.when(sides[side][0])
            def _():
                h_out(j, f, side).start()

    def take_halos(j, f, p):
        for side, rows in enumerate((low_x, high_x, low_y, high_y)):
            @pl.when(sides[side][0])
            def _():
                h_in(j, f, side).wait_recv()
                r = hxr if side < 2 else hyr
                for c in range(2):
                    p[f, c, rows, :] = r[j, f, side % 2, c].astype(F32)

    def adjoint(f):
        real = q[f, :, :, 0].reshape(512, 128)
        imag = q[f, :, :, 1].reshape(512, 128)
        acc = jnp.dot(a[f, 0], jnp.concatenate([real, imag], axis=1), preferred_element_type=F32)
        acc += jnp.dot(a[f, 1], jnp.concatenate([imag, -real], axis=1), preferred_element_type=F32)
        for x in range(32):
            for c in range(2):
                b0[f, c, pl.ds(PITCH * (x + 1), 16), :] = (
                    acc[16 * x : 16 * x + 16, 128 * c : 128 * c + 128] * inv[x]
                )
        send_edges(0, f, b0)

    @pl.loop(0, NF)
    def _(f):
        z_own(f, 0).start()
        z_own(f, 1).start()

    @pl.loop(0, NF + 3)
    def _(i):
        @pl.when(i < NF)
        def _():
            z_in(i, lax.rem(i, 2)).wait_recv()
            z_relay(i).start()

        @pl.when((i >= 1) & (i < NF + 1))
        def _():
            f = i - 1
            z_in(f, 1 - lax.rem(f, 2)).wait_recv()
            z_far(f).wait_recv()
            x_own(f, 0).start()
            x_own(f, 1).start()

        @pl.when((i >= 2) & (i < NF + 2))
        def _():
            f = i - 2
            x_in(f, lax.rem(f, 2)).wait_recv()
            x_relay(f).start()

        @pl.when(i < NF)
        def _():
            for c in range(2):
                at[i, c] = a[i, c].T

        @pl.when(i >= 3)
        def _():
            f = i - 3
            x_in(f, 1 - lax.rem(f, 2)).wait_recv()
            x_far(f).wait_recv()
            adjoint(f)

    def swept(f, c, x, p):
        base = PITCH * (x + 1)
        around = (
            p[f, c, pl.ds(base - PITCH, 16), :] + p[f, c, pl.ds(base + PITCH, 16), :]
            + p[f, c, pl.ds(base - 1, 16), :] + p[f, c, pl.ds(base + 1, 16), :]
        )
        return b0[f, c, pl.ds(base, 16), :] + kd[x] * around

    for j, (before, after) in enumerate(((b0, p1), (p1, p2))):
        @pl.loop(0, NF)
        def _(f):
            take_halos(j, f, before)
            for x in range(32):
                for c in range(2):
                    after[f, c, pl.ds(PITCH * (x + 1), 16), :] = swept(f, c, x, before)
            send_edges(j + 1, f, after)

    def forward(f):
        take_halos(2, f, p2)
        for x in range(32):
            for c in range(2):
                fh[c, pl.ds(16 * x, 16), :] = swept(f, c, x, p2).astype(BF)
        real, imag = fh[0], fh[1]
        acc = jnp.dot(at[f, 0], jnp.concatenate([real, imag], axis=1), preferred_element_type=F32)
        acc += jnp.dot(at[f, 1], jnp.concatenate([-imag, real], axis=1), preferred_element_type=F32)
        for t in range(16):
            for c in range(2):
                out[f, t % G, t // G, c] = acc[32 * t : 32 * t + 32, 128 * c : 128 * c + 128].astype(BF)

    def way(f):
        return 1 + 2 * lax.rem(f, 2)

    def back(f):
        return 3 - 2 * lax.rem(f, 2)

    def x_sum(f, kind):
        d, to, land = ((2, way(f), rxf), (back(f), back(f), rxd), (way(f), way(f), rxc))[kind]
        return remote(out.at[f, add(sy, d, G)], land.at[f], rxs.at[f, kind], rxr.at[f, kind], on_x(to))

    def z_sum(f, kind):
        d, to, land = ((2, way(f), rzf), (back(f), back(f), rzd), (way(f), way(f), rzc))[kind]
        return remote(sx_buf.at[f, add(sx, d, G)], land.at[f], rzs.at[f, kind], rzr.at[f, kind], on_z(to))

    @pl.loop(0, NF + 4)
    def _(i):
        @pl.when(i < NF)
        def _():
            forward(i)
            x_sum(i, 0).start()
            x_sum(i, 1).start()

        @pl.when((i >= 1) & (i < NF + 1))
        def _():
            f = i - 1
            x_sum(f, 0).wait_recv()
            there = add(sy, way(f), G)
            out[f, there] = (out[f, there].astype(F32) + rxf[f].astype(F32)).astype(BF)
            x_sum(f, 2).start()

        @pl.when((i >= 2) & (i < NF + 2))
        def _():
            f = i - 2
            x_sum(f, 1).wait_recv()
            x_sum(f, 2).wait_recv()
            sx_buf[f] = (out[f, sy].astype(F32) + rxd[f].astype(F32) + rxc[f].astype(F32)).astype(BF)
            z_sum(f, 0).start()
            z_sum(f, 1).start()

        @pl.when((i >= 3) & (i < NF + 3))
        def _():
            f = i - 3
            z_sum(f, 0).wait_recv()
            there = add(sx, way(f), G)
            sx_buf[f, there] = (sx_buf[f, there].astype(F32) + rzf[f].astype(F32)).astype(BF)
            z_sum(f, 2).start()

        @pl.when(i >= 4)
        def _():
            f = i - 4
            z_sum(f, 1).wait_recv()
            z_sum(f, 2).wait_recv()
            fin[f] = sx_buf[f, sx].astype(F32) + rzd[f].astype(F32) + rzc[f].astype(F32)

    for kb, chunk in enumerate(swapped([fin[i // 2, i % 2] for i in range(16)], 1)):
        r2s[kb] = chunk.astype(BF)
    for d in range(1, 16):
        a_exchange(d, r2s, r2r, bs_sem, br_sem).start()
    r2r[fq] = r2s[fq]
    for d in range(1, 16):
        a_arrival(d, r2r, bs_sem, br_sem).wait_recv()
    halves = []
    for half in range(2):
        part = swapped([r2r[8 * half + i].astype(F32) for i in range(8)], 16)
        halves.append(jnp.concatenate(part, axis=0))
    returned = jnp.dot(
        jnp.concatenate(halves, axis=1), back_ref[...], preferred_element_type=F32, precision=HIGHEST
    )

    for k in range(8):
        product = dir_ref[k] + noise_ref[...] * returned[32 * k : 32 * k + 32]
        new = res_ref[k] - step_ref[k] * product
        new_res_ref[k] = new
        total = jnp.sum(jnp.sum(new * new, axis=1, keepdims=True), axis=0, keepdims=True)
        ns[k : k + 1, :] = jnp.broadcast_to(total, (1, 128))

    def n_copy(d):
        return remote(ns, nr.at[d], ns_sem.at[d], nr_sem.at[d], in_tiles(d))

    for d in range(1, 16):
        n_copy(d).start()
    norm = ns[...]
    for d in range(1, 16):
        n_copy(d).wait_recv()
        norm += nr[d]
    norm_ref[...] = norm

    for d in range(1, 16):
        a_exchange(d, a2s, a2r, as_sem, ar_sem).wait_send()
        a_exchange(d, r2s, r2r, bs_sem, br_sem).wait_send()
        n_copy(d).wait_send()

    @pl.loop(0, NF)
    def _(f):
        for side in range(2):
            z_own(f, side).wait_send()
            x_own(f, side).wait_send()
        z_relay(f).wait_send()
        x_relay(f).wait_send()
        for kind in range(3):
            x_sum(f, kind).wait_send()
            z_sum(f, kind).wait_send()
        for j in range(3):
            for side in range(4):
                @pl.when(sides[side][0])
                def _():
                    h_out(j, f, side).wait_send()


def on_device(
    spectra, noise_weight, class_map, class_kappa, solution, residual, direction, step_length, old_norm
):
    forward_table, back_table = tables(128, 256, NF)
    vmem = pl.BlockSpec(memory_space=pltpu.VMEM)
    smem = pl.BlockSpec(memory_space=pltpu.SMEM)
    dma = pltpu.SemaphoreType.DMA
    field = pltpu.VMEM((NF, 2, 34 * PITCH, 128), F32)
    chunks = pltpu.VMEM((16, 32, 128), BF)
    x_part = pltpu.VMEM((NF, G, 2, 32, 128), BF)
    z_part = pltpu.VMEM((NF, 2, 32, 128), BF)
    new_residual, norm = pl.pallas_call(
        kernel,
        out_shape=(
            jax.ShapeDtypeStruct(residual.shape, F32),
            jax.ShapeDtypeStruct((8, 128), F32),
        ),
        in_specs=[vmem] * 4 + [smem] * 2 + [vmem] * 2 + [pl.BlockSpec(memory_space=pl.ANY)],
        out_specs=(vmem, vmem),
        scratch_shapes=[
            pltpu.VMEM((NF, 2, 512, 512), BF),
            pltpu.VMEM((NF, 2, 512, 512), BF),
            pltpu.VMEM((NF, G, G, 2, 32, 128), BF),
            field, field, field,
            pltpu.VMEM((32, 16, 128), F32), pltpu.VMEM((32, 16, 128), F32),
            pltpu.VMEM((NF, G, G, 2, 32, 128), BF),
            x_part,
            pltpu.VMEM((NF, 2, 32, 128), F32),
            chunks, chunks, chunks, chunks,
            pltpu.VMEM((3, NF, 2, 2, 16, 128), BF), pltpu.VMEM((3, NF, 2, 2, 16, 128), BF),
            pltpu.VMEM((3, NF, 2, 2, 32, 128), BF), pltpu.VMEM((3, NF, 2, 2, 32, 128), BF),
            x_part, x_part, x_part, z_part, z_part, z_part,
            pltpu.VMEM((8, 128), F32), pltpu.VMEM((16, 8, 128), F32),
            pltpu.VMEM((2, 512, 128), BF),
            dma((NF,)),
            dma((16,)), dma((16,)), dma((16,)), dma((16,)), dma((16,)), dma((16,)),
            dma((NF, 3)), dma((NF, 3)), dma((NF, 3)), dma((NF, 3)),
            dma((3, NF, 4)), dma((3, NF, 4)),
            dma((NF, 3)), dma((NF, 3)), dma((NF, 3)), dma((NF, 3)),
        ],
        compiler_params=pltpu.CompilerParams(
            collective_id=0, has_side_effects=True, vmem_limit_bytes=62 * 1024 * 1024
        ),
        name="hessian_step",
    )(
        direction, residual, noise_weight, class_map, class_kappa, step_length,
        jnp.asarray(forward_table), jnp.asarray(back_table), spectra.reshape(NF, 2, 512, 512),
    )
    new_norm = norm[:, 0]
    new_solution = solution + step_length[:, None, None] * direction
    new_direction = new_residual + (new_norm / old_norm)[:, None, None] * direction
    return (new_solution, new_residual, new_direction, new_norm)


def solution(mesh):
    columns = P("fq", ("sx", "sy"), None)
    return jax.shard_map(
        on_device,
        mesh=mesh,
        in_specs=(
            P("fq", None, "sx", "sy", None), P(("sx", "sy"), None), P("sx", "sy"), P(),
            columns, columns, columns, P("fq"), P("fq"),
        ),
        out_specs=(columns, columns, columns, P("fq")),
        check_vma=False,
    )
```

```python
import functools
import math

import jax
import jax.numpy as jnp
import numpy as np
from jax import lax
from jax.experimental import pallas as pl
from jax.experimental.pallas import tpu as pltpu
from jax.sharding import PartitionSpec as P

MESH = pl.DeviceIdType.MESH
HIGHEST = lax.Precision.HIGHEST
BF, F32 = jnp.bfloat16, jnp.float32
PITCH = 24
NF = 8
G = 4
FAR, PASS, PASS_FAR, ADJOINT, SWEEP1, SWEEP2, FORWARD, X_RELAY, X_TOTAL, Z_RELAY = 1, 2, 3, 5, 8, 11, 14, 17, 20, 23
OWN_ROW, OWN_RELAY = NF + X_RELAY - 1, NF + X_TOTAL - 1


def tables(freq_count, time_steps, per_block):
    freq = np.arange(freq_count)
    phase = (freq[:, None] * np.arange(time_steps)[None, :] % time_steps) * (2.0 * math.pi / time_steps)
    factor = 1.0 / math.sqrt(time_steps)
    both = np.stack([np.cos(phase), -np.sin(phase)], axis=1) * factor
    doubled = both * np.where(freq == 0, 1.0, 2.0)[:, None, None]
    forward = both.reshape(2 * freq_count, time_steps).T
    back = doubled.reshape(2 * freq_count, time_steps)
    return forward.astype(np.float32), back.astype(np.float32)


def swapped(arrays, unit):
    arrays = list(arrays)
    lane = lax.broadcasted_iota(jnp.int32, arrays[0].shape, 1)
    bit = 1
    while bit < len(arrays):
        here = ((lane // unit) & bit) != 0
        for i in range(len(arrays)):
            if i & bit == 0:
                a, c = arrays[i], arrays[i | bit]
                arrays[i] = jnp.where(here, pltpu.roll(c, bit * unit, 1), a)
                arrays[i | bit] = jnp.where(here, c, pltpu.roll(a, 128 - bit * unit, 1))
        bit *= 2
    return arrays


def remote(src, dst, send, recv, device):
    return pltpu.make_async_remote_copy(
        src_ref=src, dst_ref=dst, send_sem=send, recv_sem=recv, device_id=device, device_id_type=MESH
    )


def kernel(
    dir_hbm, noise_hbm, fwd_hbm, map_hbm, back_hbm, res_hbm, kap_ref, step_ref, spectra_ref,
    delta_hbm, norm_ref,
    dir_ref, noise_ref, fwd_ref, map_ref, back_ref, res_ref, delta, in_sem, out_sem,
    a, at, q, b0, p1, p2, kd, inv, out, sx_buf, fin, a2s, a2r, r2s, r2r,
    hxs, hxr, hys, hyr, rxf, rxd, rxc, rzf, rzd, rzc, ns, nr, fh,
    a_sem, as_sem, ar_sem, bs_sem, br_sem, ns_sem, nr_sem,
    zs, zr, xs, xr, hs, hr, rxs, rxr, rzs, rzr,
):
    sx, sy, fq = lax.axis_index("sx"), lax.axis_index("sy"), lax.axis_index("fq")
    tile = sx * G + sy

    def add(i, d, n):
        return lax.rem(i + d + n, n)

    def on_z(d):
        return (add(sx, d, G), sy, fq)

    def on_x(d):
        return (sx, add(sy, d, G), fq)

    def in_fq(d):
        return (sx, sy, add(fq, d, 16))

    def in_tiles(d):
        other = add(tile, d, 16)
        return (other // G, lax.rem(other, G), fq)

    barrier = pltpu.get_barrier_semaphore()
    for d in range(1, 16):
        pl.semaphore_signal(barrier, inc=1, device_id=in_fq(d), device_id_type=MESH)
        pl.semaphore_signal(barrier, inc=1, device_id=in_tiles(d), device_id_type=MESH)

    loads = [
        pltpu.make_async_copy(src, dst, in_sem.at[i])
        for i, (src, dst) in enumerate((
            (dir_hbm, dir_ref), (noise_hbm, noise_ref), (fwd_hbm, fwd_ref),
            (map_hbm, map_ref), (back_hbm, back_ref), (res_hbm, res_ref),
        ))
    ]
    for load in loads:
        load.start()

    def a_copy(f):
        return pltpu.make_async_copy(spectra_ref.at[f], a.at[f], a_sem.at[f])

    for load in loads[:3]:
        load.wait()
    for f in range(NF):
        a_copy(f).start()

    weighted = (dir_ref[...] * noise_ref[...][None]).reshape(256, 256)
    spec = jnp.dot(weighted, fwd_ref[...], preferred_element_type=F32, precision=HIGHEST)
    for half in range(2):
        part = [spec[32 * k : 32 * k + 32, 128 * half : 128 * half + 128] for k in range(8)]
        for i, chunk in enumerate(swapped(part, 16)):
            a2s[8 * half + i] = chunk.astype(BF)
    pl.semaphore_wait(barrier, 30)

    def a_exchange(d, src, dst, ss, rs):
        peer = in_fq(d)
        return remote(src.at[peer[2]], dst.at[fq], ss.at[d], rs.at[d], peer)

    def a_arrival(d, dst, ss, rs):
        peer = in_fq(-d)
        return remote(dst.at[peer[2]], dst.at[peer[2]], ss.at[d], rs.at[d], peer)

    for d in range(1, 16):
        a_exchange(d, a2s, a2r, as_sem, ar_sem).start()
    a2r[fq] = a2s[fq]

    loads[3].wait()
    classes = map_ref[...]
    kappa = jnp.zeros(classes.shape, F32)
    for c in range(8):
        kappa = jnp.where(classes == c, kap_ref[c], kappa)
    scale = 1.0 / (1.0 + 4.0 * kappa)
    ratio = scale * kappa
    for x in range(32):
        inv[x] = jnp.broadcast_to(scale[:, x : x + 1], (16, 128))
        kd[x] = jnp.broadcast_to(ratio[:, x : x + 1], (16, 128))

    zero_x = jnp.zeros((NF, 2, 16, 128), F32)
    zero_y = jnp.zeros((32, 128), F32)
    low_x, high_x = pl.ds(0, 16), pl.ds(33 * PITCH, 16)
    low_y, high_y = pl.ds(PITCH - 1, 32, stride=PITCH), pl.ds(PITCH + 16, 32, stride=PITCH)
    padded = (b0, p1, p2)

    @pl.when(sx == 0)
    def _():
        for p in padded:
            p[:, :, low_x, :] = zero_x

    @pl.when(sx == G - 1)
    def _():
        for p in padded:
            p[:, :, high_x, :] = zero_x

    @pl.when(sy == 0)
    def _():
        @pl.loop(0, NF)
        def _(f):
            for p in padded:
                for c in range(2):
                    p[f, c, low_y, :] = zero_y

    @pl.when(sy == G - 1)
    def _():
        @pl.loop(0, NF)
        def _(f):
            for p in padded:
                for c in range(2):
                    p[f, c, high_y, :] = zero_y

    for f in range(NF):
        a_copy(f).wait()
    for d in range(1, 16):
        a_arrival(d, a2r, as_sem, ar_sem).wait_recv()
    for i, block in enumerate(swapped([a2r[kb].astype(F32) for kb in range(16)], 1)):
        q[i // 2, sx, sy, i % 2] = block.astype(BF)

    def z_own(f, side):
        return remote(q.at[f, sx, sy], q.at[f, sx, sy], zs.at[f, side], zr.at[f, side], on_z(1 - 2 * side))

    def z_relay(f):
        side = lax.rem(f, 2)
        block = q.at[f, add(sx, 3 + 2 * side, G), sy]
        return remote(block, block, zs.at[f, 2], zr.at[f, 2], on_z(1 + 2 * side))

    def z_in(f, side):
        block = q.at[f, add(sx, 3 + 2 * side, G), sy]
        return remote(block, block, zs.at[f, side], zr.at[f, side], on_z(1))

    def z_far(f):
        block = q.at[f, add(sx, 2, G), sy]
        return remote(block, block, zs.at[f, 2], zr.at[f, 2], on_z(1))

    def x_own(f, row, side):
        block = q.at[f, row, sy]
        return remote(block, block, xs.at[f, side, row], xr.at[f, side, row], on_x(1 - 2 * side))

    def x_relay(f, row):
        side = lax.rem(f, 2)
        block = q.at[f, row, add(sy, 3 + 2 * side, G)]
        return remote(block, block, xs.at[f, 2, row], xr.at[f, 2, row], on_x(1 + 2 * side))

    def x_in(f, row, side):
        block = q.at[f, row, add(sy, 3 + 2 * side, G)]
        return remote(block, block, xs.at[f, side, row], xr.at[f, side, row], on_x(1))

    def x_far(f, row):
        block = q.at[f, row, add(sy, 2, G)]
        return remote(block, block, xs.at[f, 2, row], xr.at[f, 2, row], on_x(1))

    sides = ((sx > 0, on_z(-1)), (sx < G - 1, on_z(1)), (sy > 0, on_x(-1)), (sy < G - 1, on_x(1)))

    def h_out(j, f, side):
        s, r = (hxs, hxr) if side < 2 else (hys, hyr)
        return remote(
            s.at[j, f, side % 2], r.at[j, f, 1 - side % 2],
            hs.at[j, f, side], hr.at[j, f, side ^ 1], sides[side][1],
        )

    def h_in(j, f, side):
        r = hxr if side < 2 else hyr
        return remote(
            r.at[j, f, side % 2], r.at[j, f, side % 2], hs.at[j, f, side], hr.at[j, f, side], sides[side][1]
        )

    def send_edges(j, f, p):
        for c in range(2):
            hxs[j, f, 0, c] = p[f, c, pl.ds(PITCH, 16), :].astype(BF)
            hxs[j, f, 1, c] = p[f, c, pl.ds(32 * PITCH, 16), :].astype(BF)
            hys[j, f, 0, c] = p[f, c, pl.ds(PITCH, 32, stride=PITCH), :].astype(BF)
            hys[j, f, 1, c] = p[f, c, pl.ds(PITCH + 15, 32, stride=PITCH), :].astype(BF)
        for side in range(4):
            @pl.when(sides[side][0])
            def _():
                h_out(j, f, side).start()

    def take_halos(j, f, p):
        for side, rows in enumerate((low_x, high_x, low_y, high_y)):
            @pl.when(sides[side][0])
            def _():
                h_in(j, f, side).wait_recv()
                r = hxr if side < 2 else hyr
                for c in range(2):
                    p[f, c, rows, :] = r[j, f, side % 2, c].astype(F32)

    def adjoint(f):
        real = q[f, :, :, 0].reshape(512, 128)
        imag = q[f, :, :, 1].reshape(512, 128)
        acc = jnp.dot(a[f, 0], jnp.concatenate([real, imag], axis=1), preferred_element_type=F32)
        acc += jnp.dot(a[f, 1], jnp.concatenate([imag, -real], axis=1), preferred_element_type=F32)
        for x in range(32):
            for c in range(2):
                b0[f, c, pl.ds(PITCH * (x + 1), 16), :] = (
                    acc[16 * x : 16 * x + 16, 128 * c : 128 * c + 128] * inv[x]
                )
        send_edges(0, f, b0)

    @pl.loop(0, NF)
    def _(f):
        for side in range(2):
            z_own(f, side).start()
        for side in range(2):
            x_own(f, sx, side).start()

    def pass_on(f, row):
        x_in(f, row, lax.rem(f, 2)).wait_recv()
        x_relay(f, row).start()

    def row_of(side):
        return add(sx, 3 + 2 * side, G)

    def swept(f, c, x, p):
        base = PITCH * (x + 1)
        around = (
            p[f, c, pl.ds(base - PITCH, 16), :] + p[f, c, pl.ds(base + PITCH, 16), :]
            + p[f, c, pl.ds(base - 1, 16), :] + p[f, c, pl.ds(base + 1, 16), :]
        )
        return b0[f, c, pl.ds(base, 16), :] + kd[x] * around

    def sweep(j, f, before, after):
        take_halos(j, f, before)
        for x in range(32):
            for c in range(2):
                after[f, c, pl.ds(PITCH * (x + 1), 16), :] = swept(f, c, x, before)
        send_edges(j + 1, f, after)

    def forward(f):
        take_halos(2, f, p2)
        for x in range(32):
            for c in range(2):
                fh[c, pl.ds(16 * x, 16), :] = swept(f, c, x, p2).astype(BF)
        real, imag = fh[0], fh[1]
        acc = jnp.dot(at[f, 0], jnp.concatenate([real, imag], axis=1), preferred_element_type=F32)
        acc += jnp.dot(at[f, 1], jnp.concatenate([-imag, real], axis=1), preferred_element_type=F32)
        for t in range(16):
            for c in range(2):
                out[f, t % G, lax.rem(t // G + G - sx, G), c] = acc[32 * t : 32 * t + 32, 128 * c : 128 * c + 128].astype(BF)

    def way(f):
        return 1 + 2 * lax.rem(f, 2)

    def back(f):
        return 3 - 2 * lax.rem(f, 2)

    rest = (pl.ds(1, G - 1), pl.ds(0, 1))

    def x_sum(f, kind, part):
        d, to, land = ((2, way(f), rxf), (back(f), back(f), rxd), (way(f), way(f), rxc))[kind]
        return remote(
            out.at[f, add(sy, d, G), rest[part]], land.at[f, rest[part]],
            rxs.at[f, kind, part], rxr.at[f, kind, part], on_x(to),
        )

    def z_sum(f, kind):
        d, to, land = ((2, way(f), rzf), (back(f), back(f), rzd), (way(f), way(f), rzc))[kind]
        return remote(sx_buf.at[f, d], land.at[f], rzs.at[f, kind], rzr.at[f, kind], on_z(to))

    def x_relay_sum(f, part):
        x_sum(f, 0, part).wait_recv()
        there, rows = add(sy, way(f), G), rest[part]
        out[f, there, rows] = (out[f, there, rows].astype(F32) + rxf[f, rows].astype(F32)).astype(BF)
        x_sum(f, 2, part).start()

    def x_total(f, part):
        x_sum(f, 1, part).wait_recv()
        x_sum(f, 2, part).wait_recv()
        rows = rest[part]
        return out[f, sy, rows].astype(F32) + rxd[f, rows].astype(F32) + rxc[f, rows].astype(F32)

    @pl.loop(0, NF + Z_RELAY)
    def _(i):
        def stage(first):
            return pl.when((i >= first) & (i < first + NF))

        @stage(0)
        def _():
            first = lax.rem(i, 2)
            z_in(i, first).wait_recv()
            z_relay(i).start()
            for side in range(2):
                x_own(i, row_of(first), side).start()
            z_in(i, 1 - first).wait_recv()
            for side in range(2):
                x_own(i, row_of(1 - first), side).start()

        @stage(FAR)
        def _():
            f = i - FAR
            pass_on(f, sx)
            z_far(f).wait_recv()
            for side in range(2):
                x_own(f, add(sx, 2, G), side).start()

        @stage(PASS)
        def _():
            f = i - PASS
            first = lax.rem(f, 2)
            pass_on(f, row_of(first))
            pass_on(f, row_of(1 - first))

        @stage(PASS_FAR)
        def _():
            pass_on(i - PASS_FAR, add(sx, 2, G))

        @stage(0)
        def _():
            for c in range(2):
                at[i, c] = a[i, c].T

        @stage(ADJOINT)
        def _():
            f = i - ADJOINT
            for row in range(G):
                x_in(f, row, 1 - lax.rem(f, 2)).wait_recv()
                x_far(f, row).wait_recv()
            adjoint(f)

        @stage(SWEEP1)
        def _():
            sweep(0, i - SWEEP1, b0, p1)

        @stage(SWEEP2)
        def _():
            sweep(1, i - SWEEP2, p1, p2)

        @stage(FORWARD)
        def _():
            f = i - FORWARD
            forward(f)
            x_sum(f, 0, 0).start()
            x_sum(f, 1, 0).start()

        @stage(X_RELAY)
        def _():
            x_relay_sum(i - X_RELAY, 0)

        @pl.when(i == OWN_ROW)
        def _():
            @pl.loop(0, NF)
            def _(f):
                x_sum(f, 0, 1).start()
                x_sum(f, 1, 1).start()

        @stage(X_TOTAL)
        def _():
            f = i - X_TOTAL
            sx_buf[f, rest[0]] = x_total(f, 0).astype(BF)
            z_sum(f, 0).start()
            z_sum(f, 1).start()

        @pl.when(i == OWN_RELAY)
        def _():
            @pl.loop(0, NF)
            def _(f):
                x_relay_sum(f, 1)

        @stage(Z_RELAY)
        def _():
            f = i - Z_RELAY
            z_sum(f, 0).wait_recv()
            sx_buf[f, way(f)] = (sx_buf[f, way(f)].astype(F32) + rzf[f].astype(F32)).astype(BF)
            z_sum(f, 2).start()

    @pl.loop(0, NF)
    def _(f):
        own = x_total(f, 1)[0]
        z_sum(f, 1).wait_recv()
        z_sum(f, 2).wait_recv()
        fin[f] = own + rzd[f].astype(F32) + rzc[f].astype(F32)

    for kb, chunk in enumerate(swapped([fin[i // 2, i % 2] for i in range(16)], 1)):
        r2s[kb] = chunk.astype(BF)
    for d in range(1, 16):
        a_exchange(d, r2s, r2r, bs_sem, br_sem).start()
    r2r[fq] = r2s[fq]
    for d in range(1, 16):
        a_arrival(d, r2r, bs_sem, br_sem).wait_recv()
    for load in loads[4:]:
        load.wait()
    halves = []
    for half in range(2):
        part = swapped([r2r[8 * half + i].astype(F32) for i in range(8)], 16)
        halves.append(jnp.concatenate(part, axis=0))
    returned = jnp.dot(
        jnp.concatenate(halves, axis=1), back_ref[...], preferred_element_type=F32, precision=HIGHEST
    )

    for k in range(8):
        less = step_ref[k] * (dir_ref[k] + noise_ref[...] * returned[32 * k : 32 * k + 32])
        delta[k] = less
        new = res_ref[k] - less
        total = jnp.sum(jnp.sum(new * new, axis=1, keepdims=True), axis=0, keepdims=True)
        ns[k : k + 1, :] = jnp.broadcast_to(total, (1, 128))
    leave = pltpu.make_async_copy(delta, delta_hbm, out_sem)

    def n_copy(d):
        return remote(ns, nr.at[d], ns_sem.at[d], nr_sem.at[d], in_tiles(d))

    for d in range(1, 16):
        n_copy(d).start()
    leave.start()
    norm = ns[...]
    for d in range(1, 16):
        n_copy(d).wait_recv()
        norm += nr[d]
    for k in range(8):
        norm_ref[k] = norm[k, 0]
    leave.wait()

    for d in range(1, 16):
        a_exchange(d, a2s, a2r, as_sem, ar_sem).wait_send()
        a_exchange(d, r2s, r2r, bs_sem, br_sem).wait_send()
        n_copy(d).wait_send()

    @pl.loop(0, NF)
    def _(f):
        for side in range(2):
            z_own(f, side).wait_send()
            for row in range(G):
                x_own(f, row, side).wait_send()
        z_relay(f).wait_send()
        for row in range(G):
            x_relay(f, row).wait_send()
        for kind in range(3):
            z_sum(f, kind).wait_send()
            for part in range(2):
                x_sum(f, kind, part).wait_send()
        for j in range(3):
            for side in range(4):
                @pl.when(sides[side][0])
                def _():
                    h_out(j, f, side).wait_send()


def on_device(
    spectra, noise_weight, class_map, class_kappa, solution, residual, direction, step_length, old_norm
):
    forward_table, back_table = tables(128, 256, NF)
    smem = pl.BlockSpec(memory_space=pltpu.SMEM)
    dma = pltpu.SemaphoreType.DMA
    field = pltpu.VMEM((NF, 2, 34 * PITCH, 128), F32)
    chunks = pltpu.VMEM((16, 32, 128), BF)
    x_part = pltpu.VMEM((NF, G, 2, 32, 128), BF)
    z_part = pltpu.VMEM((NF, 2, 32, 128), BF)
    hbm = pl.BlockSpec(memory_space=pl.ANY)
    delta, new_norm = pl.pallas_call(
        kernel,
        out_shape=(
            jax.ShapeDtypeStruct(residual.shape, F32),
            jax.ShapeDtypeStruct((8,), F32),
        ),
        in_specs=[hbm] * 6 + [smem] * 2 + [hbm],
        out_specs=(hbm, smem),
        scratch_shapes=[
            pltpu.VMEM(direction.shape, F32), pltpu.VMEM((32, 256), F32), pltpu.VMEM((256, 256), F32),
            pltpu.VMEM((16, 32), jnp.int32), pltpu.VMEM((256, 256), F32), pltpu.VMEM(direction.shape, F32),
            pltpu.VMEM(direction.shape, F32), dma((6,)), dma,
            pltpu.VMEM((NF, 2, 512, 512), BF),
            pltpu.VMEM((NF, 2, 512, 512), BF),
            pltpu.VMEM((NF, G, G, 2, 32, 128), BF),
            field, field, field,
            pltpu.VMEM((32, 16, 128), F32), pltpu.VMEM((32, 16, 128), F32),
            pltpu.VMEM((NF, G, G, 2, 32, 128), BF),
            x_part,
            pltpu.VMEM((NF, 2, 32, 128), F32),
            chunks, chunks, chunks, chunks,
            pltpu.VMEM((3, NF, 2, 2, 16, 128), BF), pltpu.VMEM((3, NF, 2, 2, 16, 128), BF),
            pltpu.VMEM((3, NF, 2, 2, 32, 128), BF), pltpu.VMEM((3, NF, 2, 2, 32, 128), BF),
            x_part, x_part, x_part, z_part, z_part, z_part,
            pltpu.VMEM((8, 128), F32), pltpu.VMEM((16, 8, 128), F32),
            pltpu.VMEM((2, 512, 128), BF),
            dma((NF,)),
            dma((16,)), dma((16,)), dma((16,)), dma((16,)), dma((16,)), dma((16,)),
            dma((NF, 3)), dma((NF, 3)), dma((NF, 3, G)), dma((NF, 3, G)),
            dma((3, NF, 4)), dma((3, NF, 4)),
            dma((NF, 3, 2)), dma((NF, 3, 2)), dma((NF, 3)), dma((NF, 3)),
        ],
        compiler_params=pltpu.CompilerParams(
            collective_id=0, has_side_effects=True, vmem_limit_bytes=62 * 1024 * 1024
        ),
        name="hessian_step",
    )(
        direction, noise_weight, jnp.asarray(forward_table), class_map.T, jnp.asarray(back_table), residual,
        class_kappa, step_length, spectra.reshape(NF, 2, 512, 512),
    )
    new_residual = residual - delta
    new_solution = solution + step_length[:, None, None] * direction
    new_direction = new_residual + (new_norm / old_norm)[:, None, None] * direction
    return (new_solution, new_residual, new_direction, new_norm)


def solution(mesh):
    columns = P("fq", ("sx", "sy"), None)
    return jax.shard_map(
        on_device,
        mesh=mesh,
        in_specs=(
            P("fq", None, "sx", "sy", None), P(("sx", "sy"), None), P("sx", "sy"), P(),
            columns, columns, columns, P("fq"), P("fq"),
        ),
        out_specs=(columns, columns, columns, P("fq")),
        check_vma=False,
    )
```

```python
import functools
import math

import jax
import jax.numpy as jnp
import numpy as np
from jax import lax
from jax.experimental import pallas as pl
from jax.experimental.pallas import tpu as pltpu
from jax.sharding import PartitionSpec as P

MESH = pl.DeviceIdType.MESH
HIGHEST = lax.Precision.HIGHEST
BF, F32 = jnp.bfloat16, jnp.float32
PITCH = 24
NF = 8
G = 4
GATHER_TURNED, SUM_TURNED = (3,), (1, 4)
FAR, PASS, PASS_FAR, ADJOINT, FORWARD, X_RELAY, X_TOTAL = 1, 2, 4, 6, 9, 12, 15
OWN_ROW, OWN_RELAY = NF + X_RELAY - 1, NF + X_TOTAL - 1
DEEP = 3
ROWS = PITCH * (32 + 2 * DEEP + 2)


def tables(freq_count, time_steps, per_block):
    freq = np.arange(freq_count)
    phase = (freq[:, None] * np.arange(time_steps)[None, :] % time_steps) * (2.0 * math.pi / time_steps)
    factor = 1.0 / math.sqrt(time_steps)
    both = np.stack([np.cos(phase), -np.sin(phase)], axis=1) * factor
    doubled = both * np.where(freq == 0, 1.0, 2.0)[:, None, None]
    forward = both.reshape(2 * freq_count, time_steps).T
    back = doubled.reshape(2 * freq_count, time_steps)
    return forward.astype(np.float32), back.astype(np.float32)


def swapped(arrays, unit):
    arrays = list(arrays)
    lane = lax.broadcasted_iota(jnp.int32, arrays[0].shape, 1)
    bit = 1
    while bit < len(arrays):
        here = ((lane // unit) & bit) != 0
        for i in range(len(arrays)):
            if i & bit == 0:
                a, c = arrays[i], arrays[i | bit]
                arrays[i] = jnp.where(here, pltpu.roll(c, bit * unit, 1), a)
                arrays[i | bit] = jnp.where(here, c, pltpu.roll(a, 128 - bit * unit, 1))
        bit *= 2
    return arrays


def row_at(x, y):
    return PITCH * (x + DEEP + 1) + y


def remote(src, dst, send, recv, device):
    return pltpu.make_async_remote_copy(
        src_ref=src, dst_ref=dst, send_sem=send, recv_sem=recv, device_id=device, device_id_type=MESH
    )


def kernel(
    dir_hbm, noise_hbm, fwd_hbm, map_hbm, back_hbm, res_hbm, kap_ref, step_ref, old_ref, spectra_ref,
    delta_hbm, norm_ref, ratio_ref,
    dir_ref, noise_ref, fwd_ref, map_ref, back_ref, res_ref, delta, in_sem, out_sem,
    a, at, q, b0, p1, p2, kd, inv, out, sx_buf, fin, a2s, a2r, r2s, r2r,
    hxs, hxr, hys, hyr, hcs, hcr, mine, near, rxf, rxd, rxc, rz, ns, nr, fh,
    a_sem, as_sem, ar_sem, bs_sem, br_sem, ns_sem, nr_sem,
    zs, zr, xs, xr, hs, hr, ms, mr, rxs, rxr, rzs, rzr,
):
    sx, sy, fq = lax.axis_index("sx"), lax.axis_index("sy"), lax.axis_index("fq")
    tile = sx * G + sy

    def add(i, d, n):
        return lax.rem(i + d + n, n)

    def on_z(d):
        return (add(sx, d, G), sy, fq)

    def on_x(d):
        return (sx, add(sy, d, G), fq)

    def in_fq(d):
        return (sx, sy, add(fq, d, 16))

    def in_tiles(d):
        other = add(tile, d, 16)
        return (other // G, lax.rem(other, G), fq)

    barrier = pltpu.get_barrier_semaphore()
    for d in range(1, 16):
        pl.semaphore_signal(barrier, inc=1, device_id=in_fq(d), device_id_type=MESH)
        pl.semaphore_signal(barrier, inc=1, device_id=in_tiles(d), device_id_type=MESH)

    loads = [
        pltpu.make_async_copy(src, dst, in_sem.at[i])
        for i, (src, dst) in enumerate((
            (dir_hbm, dir_ref), (noise_hbm, noise_ref), (fwd_hbm, fwd_ref),
            (map_hbm, map_ref), (back_hbm, back_ref), (res_hbm, res_ref),
        ))
    ]
    for load in loads:
        load.start()

    def a_copy(f):
        return pltpu.make_async_copy(spectra_ref.at[f], a.at[f], a_sem.at[f])

    for load in loads[:3]:
        load.wait()
    for f in range(NF):
        a_copy(f).start()

    weighted = (dir_ref[...] * noise_ref[...][None]).reshape(256, 256)
    spec = jnp.dot(weighted, fwd_ref[...], preferred_element_type=F32, precision=HIGHEST)
    for half in range(2):
        part = [spec[32 * k : 32 * k + 32, 128 * half : 128 * half + 128] for k in range(8)]
        for i, chunk in enumerate(swapped(part, 16)):
            a2s[8 * half + i] = chunk.astype(BF)
    pl.semaphore_wait(barrier, 30)

    def a_exchange(d, src, dst, ss, rs):
        peer = in_fq(d)
        return remote(src.at[peer[2]], dst.at[fq], ss.at[d], rs.at[d], peer)

    def a_arrival(d, dst, ss, rs):
        peer = in_fq(-d)
        return remote(dst.at[peer[2]], dst.at[peer[2]], ss.at[d], rs.at[d], peer)

    for d in range(1, 16):
        a_exchange(d, a2s, a2r, as_sem, ar_sem).start()
    a2r[fq] = a2s[fq]

    loads[3].wait()
    classes = map_ref[...]
    kappa = jnp.zeros(classes.shape, F32)
    for c in range(8):
        kappa = jnp.where(classes == c, kap_ref[c], kappa)
    scale = 1.0 / (1.0 + 4.0 * kappa)
    ratio = scale * kappa
    mine[...] = jnp.concatenate([ratio, jnp.zeros((16, 96), F32)], axis=1)
    for x in range(32):
        inv[x] = jnp.broadcast_to(scale[:, x : x + 1], (16, 128))

    around = ((-1, 0), (1, 0), (0, -1), (0, 1), (-1, -1), (1, 1), (-1, 1), (1, -1))

    def there_is(i):
        dz, dx = around[i]
        return (sx + dz >= 0) & (sx + dz < G) & (sy + dx >= 0) & (sy + dx < G)

    def tile_at(i):
        dz, dx = around[i]
        return (add(sx, dz, G), add(sy, dx, G), fq)

    def m_copy(i):
        return remote(mine, near.at[i ^ 1], ms.at[i], mr.at[i ^ 1], tile_at(i))

    def m_in(i):
        return remote(near.at[i], near.at[i], ms.at[i], mr.at[i], tile_at(i))

    for i in range(8):
        @pl.when(there_is(i))
        def _():
            m_copy(i).start()

        @pl.when(jnp.logical_not(there_is(i)))
        def _():
            near[i] = jnp.zeros((16, 128), F32)

    @pl.loop(0, NF)
    def _(f):
        b0[f] = jnp.zeros((2, ROWS, 128), F32)

    for f in range(NF):
        a_copy(f).wait()
    for d in range(1, 16):
        a_arrival(d, a2r, as_sem, ar_sem).wait_recv()
    for i, block in enumerate(swapped([a2r[kb].astype(F32) for kb in range(16)], 1)):
        q[i // 2, sx, sy, i % 2] = block.astype(BF)

    def order_of(freqs):
        def pick(f, straight, other):
            turned = sum(((f == t).astype(jnp.int32) for t in freqs), jnp.int32(0))
            return straight + turned * (other - straight)

        def along(f, d, second):
            on_sx = pick(f, 0, d) if second else pick(f, d, 0)
            return (add(sx, on_sx, G), add(sy, d - on_sx, G), fq)

        def ones(f, d):
            return add(pick(f, sx, sy), d, G)

        def twos(f, d):
            return add(pick(f, sy, sx), d, G)

        return pick, along, ones, twos

    pick, along, ones, twos = order_of(GATHER_TURNED)
    s_pick, s_along, s_ones, s_twos = order_of(SUM_TURNED)

    def block_at(f, one, two):
        return q.at[f, pick(f, one, two), pick(f, two, one)]

    def g_copy(f, block, send, recv, d, second):
        return remote(block, block, send, recv, along(f, d, second))

    def z_own(f, side):
        return g_copy(f, q.at[f, sx, sy], zs.at[f, side], zr.at[f, side], 1 + 2 * side, False)

    def z_in(f, side):
        block = block_at(f, ones(f, 3 + 2 * side), twos(f, 0))
        return g_copy(f, block, zs.at[f, side], zr.at[f, side], 1, False)

    def z_across(f):
        return g_copy(f, q.at[f, sx, sy], zs.at[f, 2], zr.at[f, 2], 2, False)

    def z_far(f):
        block = block_at(f, ones(f, 2), twos(f, 0))
        return g_copy(f, block, zs.at[f, 2], zr.at[f, 2], 2, False)

    def x_own(f, row, side):
        block = block_at(f, row, twos(f, 0))
        return g_copy(f, block, xs.at[f, side, row], xr.at[f, side, row], 1 + 2 * side, True)

    def x_relay(f, row):
        side = lax.rem(f, 2)
        block = block_at(f, row, twos(f, 3 + 2 * side))
        return g_copy(f, block, xs.at[f, 2, row], xr.at[f, 2, row], 1 + 2 * side, True)

    def x_in(f, row, side):
        block = block_at(f, row, twos(f, 3 + 2 * side))
        return g_copy(f, block, xs.at[f, side, row], xr.at[f, side, row], 1, True)

    def x_far(f, row):
        block = block_at(f, row, twos(f, 2))
        return g_copy(f, block, xs.at[f, 2, row], xr.at[f, 2, row], 1, True)

    def h_bufs(i):
        return (hxs, hxr, i) if i < 2 else (hys, hyr, i - 2) if i < 4 else (hcs, hcr, i - 4)

    def h_out(f, i):
        s, r, k = h_bufs(i)
        return remote(s.at[f, k], r.at[f, k ^ 1], hs.at[f, i], hr.at[f, i ^ 1], tile_at(i))

    def h_in(f, i):
        _, r, k = h_bufs(i)
        return remote(r.at[f, k], r.at[f, k], hs.at[f, i], hr.at[f, i], tile_at(i))

    def corner(i, inside):
        dz, dx = around[i]
        x0 = (0 if dz < 0 else 30) if inside else (-2 if dz < 0 else 32)
        y0 = (0 if dx < 0 else 14) if inside else (-2 if dx < 0 else 16)
        return [(4 * c + 2 * m + n, c, row_at(x0 + m, y0 + n)) for c in range(2) for m in range(2) for n in range(2)]

    def send_edges(f):
        for c in range(2):
            for m in range(DEEP):
                hxs[f, 0, c, m] = b0[f, c, pl.ds(row_at(m, 0), 16), :].astype(BF)
                hxs[f, 1, c, m] = b0[f, c, pl.ds(row_at(32 - DEEP + m, 0), 16), :].astype(BF)
                hys[f, 0, c, m] = b0[f, c, pl.ds(row_at(0, m), 32, stride=PITCH), :].astype(BF)
                hys[f, 1, c, m] = b0[f, c, pl.ds(row_at(0, 16 - DEEP + m), 32, stride=PITCH), :].astype(BF)
        for i in range(4, 8):
            for to, c, at_row in corner(i, True):
                hcs[f, i - 4, to : to + 1, :] = b0[f, c, at_row : at_row + 1, :]
        for i in range(8):
            @pl.when(there_is(i))
            def _():
                h_out(f, i).start()

    def take_halos(f):
        for i in range(8):
            @pl.when(there_is(i))
            def _():
                h_in(f, i).wait_recv()
                for c in range(2):
                    for m in range(DEEP):
                        if i < 2:
                            x = m + (-DEEP, 32)[i]
                            b0[f, c, pl.ds(row_at(x, 0), 16), :] = hxr[f, i, c, m].astype(F32)
                        elif i < 4:
                            y = m + (-DEEP, 16)[i - 2]
                            b0[f, c, pl.ds(row_at(0, y), 32, stride=PITCH), :] = hyr[f, i - 2, c, m].astype(F32)
                if i >= 4:
                    for at, c, at_row in corner(i, False):
                        b0[f, c, at_row : at_row + 1, :] = hcr[f, i - 4, at : at + 1, :]

    def adjoint(f):
        real = q[f, :, :, 0].reshape(512, 128)
        imag = q[f, :, :, 1].reshape(512, 128)
        acc = jnp.dot(a[f, 0], jnp.concatenate([real, imag], axis=1), preferred_element_type=F32)
        acc += jnp.dot(a[f, 1], jnp.concatenate([imag, -real], axis=1), preferred_element_type=F32)
        for x in range(32):
            for c in range(2):
                b0[f, c, pl.ds(row_at(x, 0), 16), :] = (
                    acc[16 * x : 16 * x + 16, 128 * c : 128 * c + 128] * inv[x]
                )
        send_edges(f)

    @pl.loop(0, NF)
    def _(f):
        for side in range(2):
            z_own(f, side).start()
        z_across(f).start()
        for side in range(2):
            x_own(f, ones(f, 0), side).start()

    for i in range(8):
        @pl.when(there_is(i))
        def _():
            m_in(i).wait_recv()
    maps = {d: near[i] for i, d in enumerate(around)}
    maps[0, 0] = mine[...]
    line = lax.broadcasted_iota(jnp.int32, (8, 128), 0)

    def cells(x, dx, rows):
        dz = -1 if x < 0 else 1 if x > 31 else 0
        x -= 32 * dz
        return jnp.broadcast_to(maps[dz, dx][rows, x : x + 1], (rows.stop - rows.start, 128))

    for x in range(-DEEP, 32 + DEEP):
        kd[pl.ds(row_at(x, 0), 16), :] = cells(x, 0, slice(0, 16))
        rim = jnp.where(line < DEEP, cells(x, 1, slice(0, 8)), 0.0)
        if x < 31 + DEEP:
            rim = jnp.where(line >= 8 - DEEP, cells(x + 1, -1, slice(8, 16)), rim)
        kd[pl.ds(row_at(x, 16), 8), :] = rim
    for start in (0, ROWS - PITCH):
        kd[pl.ds(start, PITCH), :] = jnp.zeros((PITCH, 128), F32)
    kd[pl.ds(16, 8), :] = jnp.where(line >= 8 - DEEP, cells(-DEEP, -1, slice(8, 16)), 0.0)

    def pass_on(f, row):
        x_in(f, row, lax.rem(f, 2)).wait_recv()
        x_relay(f, row).start()

    def row_of(f, side):
        return ones(f, 3 + 2 * side)

    def swept(f, c, start, size, p):
        beside = (
            p[c, pl.ds(start - PITCH, size), :] + p[c, pl.ds(start + PITCH, size), :]
            + p[c, pl.ds(start - 1, size), :] + p[c, pl.ds(start + 1, size), :]
        )
        return b0[f, c, pl.ds(start, size), :] + kd[pl.ds(start, size), :] * beside

    def sweep(f, before, after, layers):
        low = row_at(-layers, -layers) // 8 * 8
        high = -(-row_at(31 + layers, 16 + layers) // 8) * 8
        for start in range(low, high, 16):
            size = min(16, high - start)
            for c in range(2):
                after[c, pl.ds(start, size), :] = swept(f, c, start, size, before)

    def forward(f):
        take_halos(f)
        sweep(f, b0.at[f], p1, 2)
        sweep(f, p1, p2, 1)
        for x in range(32):
            for c in range(2):
                fh[c, pl.ds(16 * x, 16), :] = swept(f, c, row_at(x, 0), 16, p2).astype(BF)
        real, imag = fh[0], fh[1]
        acc = jnp.dot(at[f, 0], jnp.concatenate([real, imag], axis=1), preferred_element_type=F32)
        acc += jnp.dot(at[f, 1], jnp.concatenate([-imag, real], axis=1), preferred_element_type=F32)
        for t in range(16):
            for c in range(2):
                there = s_pick(f, t % G, t // G)
                row = lax.rem(s_pick(f, t // G, t % G) + G - s_ones(f, 0), G)
                out[f, there, row, c] = acc[32 * t : 32 * t + 32, 128 * c : 128 * c + 128].astype(BF)

    def way(f):
        return 1 + 2 * lax.rem(f, 2)

    def back(f):
        return 3 - 2 * lax.rem(f, 2)

    rest = (pl.ds(1, G - 1), pl.ds(0, 1))

    def x_sum(f, kind, part):
        d, to, land = ((2, way(f), rxf), (back(f), back(f), rxd), (way(f), way(f), rxc))[kind]
        return remote(
            out.at[f, s_twos(f, d), rest[part]], land.at[f, rest[part]],
            rxs.at[f, kind, part], rxr.at[f, kind, part], s_along(f, to, True),
        )

    def z_sum(f, d):
        return remote(sx_buf.at[f, d], rz.at[f, d], rzs.at[f, d], rzr.at[f, d], s_along(f, d, False))

    def x_relay_sum(f, part):
        x_sum(f, 0, part).wait_recv()
        there, rows = s_twos(f, way(f)), rest[part]
        out[f, there, rows] = (out[f, there, rows].astype(F32) + rxf[f, rows].astype(F32)).astype(BF)
        x_sum(f, 2, part).start()

    def x_total(f, part):
        x_sum(f, 1, part).wait_recv()
        x_sum(f, 2, part).wait_recv()
        rows = rest[part]
        return out[f, s_twos(f, 0), rows].astype(F32) + rxd[f, rows].astype(F32) + rxc[f, rows].astype(F32)

    @pl.loop(0, NF + X_TOTAL)
    def _(i):
        def stage(first):
            return pl.when((i >= first) & (i < first + NF))

        @stage(0)
        def _():
            first = lax.rem(i, 2)
            z_in(i, first).wait_recv()
            for side in range(2):
                x_own(i, row_of(i, first), side).start()
            z_in(i, 1 - first).wait_recv()
            for side in range(2):
                x_own(i, row_of(i, 1 - first), side).start()

        @stage(FAR)
        def _():
            f = i - FAR
            pass_on(f, ones(f, 0))
            z_far(f).wait_recv()
            for side in range(2):
                x_own(f, ones(f, 2), side).start()

        @stage(PASS)
        def _():
            f = i - PASS
            first = lax.rem(f, 2)
            pass_on(f, row_of(f, first))
            pass_on(f, row_of(f, 1 - first))

        @stage(PASS_FAR)
        def _():
            f = i - PASS_FAR
            pass_on(f, ones(f, 2))

        @stage(0)
        def _():
            for c in range(2):
                at[i, c] = a[i, c].T

        @stage(ADJOINT)
        def _():
            f = i - ADJOINT
            for row in range(G):
                x_in(f, row, 1 - lax.rem(f, 2)).wait_recv()
                x_far(f, row).wait_recv()
            adjoint(f)

        @stage(FORWARD)
        def _():
            f = i - FORWARD
            forward(f)
            x_sum(f, 0, 0).start()
            x_sum(f, 1, 0).start()

        @stage(X_RELAY)
        def _():
            x_relay_sum(i - X_RELAY, 0)

        @pl.when(i == OWN_ROW)
        def _():
            @pl.loop(0, NF)
            def _(f):
                x_sum(f, 0, 1).start()
                x_sum(f, 1, 1).start()

        @stage(X_TOTAL)
        def _():
            f = i - X_TOTAL
            sx_buf[f, rest[0]] = x_total(f, 0).astype(BF)
            for d in range(1, G):
                z_sum(f, d).start()

        @pl.when(i == OWN_RELAY)
        def _():
            @pl.loop(0, NF)
            def _(f):
                x_relay_sum(f, 1)

    @pl.loop(0, NF)
    def _(f):
        total = x_total(f, 1)[0]
        for d in range(1, G):
            z_sum(f, d).wait_recv()
            total += rz[f, d].astype(F32)
        fin[f] = total

    for kb, chunk in enumerate(swapped([fin[i // 2, i % 2] for i in range(16)], 1)):
        r2s[kb] = chunk.astype(BF)
    for d in range(1, 16):
        a_exchange(d, r2s, r2r, bs_sem, br_sem).start()
    r2r[fq] = r2s[fq]
    for d in range(1, 16):
        a_arrival(d, r2r, bs_sem, br_sem).wait_recv()
    for load in loads[4:]:
        load.wait()
    halves = []
    for half in range(2):
        part = swapped([r2r[8 * half + i].astype(F32) for i in range(8)], 16)
        halves.append(jnp.concatenate(part, axis=0))
    returned = jnp.dot(
        jnp.concatenate(halves, axis=1), back_ref[...], preferred_element_type=F32, precision=HIGHEST
    )

    for k in range(8):
        less = step_ref[k] * (dir_ref[k] + noise_ref[...] * returned[32 * k : 32 * k + 32])
        delta[k] = less
        new = res_ref[k] - less
        total = jnp.sum(jnp.sum(new * new, axis=1, keepdims=True), axis=0, keepdims=True)
        ns[k : k + 1, :] = jnp.broadcast_to(total, (1, 128))
    leave = pltpu.make_async_copy(delta, delta_hbm, out_sem)

    def n_copy(d):
        return remote(ns, nr.at[d], ns_sem.at[d], nr_sem.at[d], in_tiles(d))

    for d in range(1, 16):
        n_copy(d).start()
    leave.start()
    norm = ns[...]
    for d in range(1, 16):
        n_copy(d).wait_recv()
        norm += nr[d]
    column = lax.broadcasted_iota(jnp.int32, (8, 128), 0)
    old = jnp.ones((8, 128), F32)
    for k in range(8):
        old = jnp.where(column == k, old_ref[k], old)
    growth = norm / old
    for k in range(8):
        norm_ref[k] = norm[k, 0]
        ratio_ref[k] = growth[k, 0]
    leave.wait()

    for d in range(1, 16):
        a_exchange(d, a2s, a2r, as_sem, ar_sem).wait_send()
        a_exchange(d, r2s, r2r, bs_sem, br_sem).wait_send()
        n_copy(d).wait_send()

    @pl.loop(0, NF)
    def _(f):
        for side in range(2):
            z_own(f, side).wait_send()
            for row in range(G):
                x_own(f, row, side).wait_send()
        z_across(f).wait_send()
        for row in range(G):
            x_relay(f, row).wait_send()
        for d in range(1, G):
            z_sum(f, d).wait_send()
        for kind in range(3):
            for part in range(2):
                x_sum(f, kind, part).wait_send()
        for i in range(8):
            @pl.when(there_is(i))
            def _():
                h_out(f, i).wait_send()

    for i in range(8):
        @pl.when(there_is(i))
        def _():
            m_copy(i).wait_send()


def on_device(
    spectra, noise_weight, class_map, class_kappa, solution, residual, direction, step_length, old_norm
):
    forward_table, back_table = tables(128, 256, NF)
    smem = pl.BlockSpec(memory_space=pltpu.SMEM)
    dma = pltpu.SemaphoreType.DMA
    field = pltpu.VMEM((2, ROWS, 128), F32)
    chunks = pltpu.VMEM((16, 32, 128), BF)
    x_part = pltpu.VMEM((NF, G, 2, 32, 128), BF)
    hbm = pl.BlockSpec(memory_space=pl.ANY)
    delta, norm, growth = pl.pallas_call(
        kernel,
        out_shape=(
            jax.ShapeDtypeStruct(residual.shape, F32),
            jax.ShapeDtypeStruct((8,), F32),
            jax.ShapeDtypeStruct((8,), F32),
        ),
        in_specs=[hbm] * 6 + [smem] * 3 + [hbm],
        out_specs=(hbm, smem, smem),
        scratch_shapes=[
            pltpu.VMEM(direction.shape, F32), pltpu.VMEM((32, 256), F32), pltpu.VMEM((256, 256), F32),
            pltpu.VMEM((16, 32), jnp.int32), pltpu.VMEM((256, 256), F32), pltpu.VMEM(direction.shape, F32),
            pltpu.VMEM(direction.shape, F32), dma((6,)), dma,
            pltpu.VMEM((NF, 2, 512, 512), BF),
            pltpu.VMEM((NF, 2, 512, 512), BF),
            pltpu.VMEM((NF, G, G, 2, 32, 128), BF),
            pltpu.VMEM((NF, 2, ROWS, 128), F32), field, field,
            pltpu.VMEM((ROWS, 128), F32), pltpu.VMEM((32, 16, 128), F32),
            pltpu.VMEM((NF, G, G, 2, 32, 128), BF),
            x_part,
            pltpu.VMEM((NF, 2, 32, 128), F32),
            chunks, chunks, chunks, chunks,
            pltpu.VMEM((NF, 2, 2, DEEP, 16, 128), BF), pltpu.VMEM((NF, 2, 2, DEEP, 16, 128), BF),
            pltpu.VMEM((NF, 2, 2, DEEP, 32, 128), BF), pltpu.VMEM((NF, 2, 2, DEEP, 32, 128), BF),
            pltpu.VMEM((NF, 4, 8, 128), F32), pltpu.VMEM((NF, 4, 8, 128), F32),
            pltpu.VMEM((16, 128), F32), pltpu.VMEM((8, 16, 128), F32),
            x_part, x_part, x_part, x_part,
            pltpu.VMEM((8, 128), F32), pltpu.VMEM((16, 8, 128), F32),
            pltpu.VMEM((2, 512, 128), BF),
            dma((NF,)),
            dma((16,)), dma((16,)), dma((16,)), dma((16,)), dma((16,)), dma((16,)),
            dma((NF, 3)), dma((NF, 3)), dma((NF, 3, G)), dma((NF, 3, G)),
            dma((NF, 8)), dma((NF, 8)), dma((8,)), dma((8,)),
            dma((NF, 3, 2)), dma((NF, 3, 2)), dma((NF, G)), dma((NF, G)),
        ],
        compiler_params=pltpu.CompilerParams(
            collective_id=0, has_side_effects=True, vmem_limit_bytes=62 * 1024 * 1024
        ),
        name="hessian_step",
    )(
        direction, noise_weight, jnp.asarray(forward_table), class_map.T, jnp.asarray(back_table), residual,
        class_kappa, step_length, old_norm, spectra.reshape(NF, 2, 512, 512),
    )
    new_residual = residual - delta
    new_norm = jnp.maximum(norm, 0.0)
    new_solution = solution + step_length[:, None, None] * direction
    new_direction = new_residual + growth[:, None, None] * direction
    return (new_solution, new_residual, new_direction, new_norm)


def solution(mesh):
    columns = P("fq", ("sx", "sy"), None)
    return jax.shard_map(
        on_device,
        mesh=mesh,
        in_specs=(
            P("fq", None, "sx", "sy", None), P(("sx", "sy"), None), P("sx", "sy"), P(),
            columns, columns, columns, P("fq"), P("fq"),
        ),
        out_specs=(columns, columns, columns, P("fq")),
        check_vma=False,
    )
```

```python
import functools
import math

import jax
import jax.numpy as jnp
import numpy as np
from jax import lax
from jax.experimental import pallas as pl
from jax.experimental.pallas import tpu as pltpu
from jax.sharding import PartitionSpec as P

MESH = pl.DeviceIdType.MESH
HIGHEST = lax.Precision.HIGHEST
BF, F32 = jnp.bfloat16, jnp.float32
PITCH = 24
NF = 8
G = 4
GATHER_TURNED, SUM_TURNED = (3,), (0, 3)
FAR, PASS, PASS_FAR, ADJOINT, FORWARD, X_RELAY, X_TOTAL = 1, 2, 4, 6, 9, 12, 15
OWN_ROW, OWN_RELAY = NF + X_RELAY - 1, NF + X_TOTAL - 1
DEEP = 3
ROWS = PITCH * (32 + 2 * DEEP + 2)


def tables(freq_count, time_steps, per_block):
    freq = np.arange(freq_count)
    phase = (freq[:, None] * np.arange(time_steps)[None, :] % time_steps) * (2.0 * math.pi / time_steps)
    factor = 1.0 / math.sqrt(time_steps)
    both = np.stack([np.cos(phase), -np.sin(phase)], axis=1) * factor
    doubled = both * np.where(freq == 0, 1.0, 2.0)[:, None, None]
    forward = both.reshape(2 * freq_count, time_steps).T
    back = doubled.reshape(2 * freq_count, time_steps)
    return forward.astype(np.float32), back.astype(np.float32)


def swapped(arrays, unit):
    arrays = list(arrays)
    lane = lax.broadcasted_iota(jnp.int32, arrays[0].shape, 1)
    bit = 1
    while bit < len(arrays):
        here = ((lane // unit) & bit) != 0
        for i in range(len(arrays)):
            if i & bit == 0:
                a, c = arrays[i], arrays[i | bit]
                arrays[i] = jnp.where(here, pltpu.roll(c, bit * unit, 1), a)
                arrays[i | bit] = jnp.where(here, c, pltpu.roll(a, 128 - bit * unit, 1))
        bit *= 2
    return arrays


def row_at(x, y):
    return PITCH * (x + DEEP + 1) + y


def remote(src, dst, send, recv, device):
    return pltpu.make_async_remote_copy(
        src_ref=src, dst_ref=dst, send_sem=send, recv_sem=recv, device_id=device, device_id_type=MESH
    )


def kernel(
    dir_hbm, noise_hbm, fwd_hbm, map_hbm, back_hbm, res_hbm, kap_ref, step_ref, old_ref, spectra_ref,
    delta_hbm, norm_ref, ratio_ref,
    dir_ref, noise_ref, fwd_ref, map_ref, back_ref, res_ref, delta, in_sem, out_sem,
    a, at, q, b0, p1, p2, kd, inv, out, sx_buf, fin, a2s, a2r, r2s, r2r,
    hxs, hxr, hys, hyr, hcs, hcr, mine, near, rxf, rxd, rxc, rz, ns, nr, fh,
    a_sem, as_sem, ar_sem, bs_sem, br_sem, ns_sem, nr_sem,
    zs, zr, xs, xr, hs, hr, ms, mr, rxs, rxr, rzs, rzr,
):
    sx, sy, fq = lax.axis_index("sx"), lax.axis_index("sy"), lax.axis_index("fq")
    tile = sx * G + sy

    def add(i, d, n):
        return lax.rem(i + d + n, n)

    def on_z(d):
        return (add(sx, d, G), sy, fq)

    def on_x(d):
        return (sx, add(sy, d, G), fq)

    def in_fq(d):
        return (sx, sy, add(fq, d, 16))

    def in_tiles(d):
        other = add(tile, d, 16)
        return (other // G, lax.rem(other, G), fq)

    barrier = pltpu.get_barrier_semaphore()
    for d in range(1, 16):
        pl.semaphore_signal(barrier, inc=1, device_id=in_fq(d), device_id_type=MESH)
        pl.semaphore_signal(barrier, inc=1, device_id=in_tiles(d), device_id_type=MESH)

    loads = [
        pltpu.make_async_copy(src, dst, in_sem.at[i])
        for i, (src, dst) in enumerate((
            (dir_hbm, dir_ref), (noise_hbm, noise_ref), (fwd_hbm, fwd_ref),
            (map_hbm, map_ref), (back_hbm, back_ref), (res_hbm, res_ref),
        ))
    ]
    for load in loads:
        load.start()

    def a_copy(f):
        return pltpu.make_async_copy(spectra_ref.at[f], a.at[f], a_sem.at[f])

    for load in loads[:3]:
        load.wait()
    for f in range(NF):
        a_copy(f).start()

    weighted = (dir_ref[...] * noise_ref[...][None]).reshape(256, 256)
    spec = jnp.dot(weighted, fwd_ref[...], preferred_element_type=F32, precision=HIGHEST)
    for half in range(2):
        part = [spec[32 * k : 32 * k + 32, 128 * half : 128 * half + 128] for k in range(8)]
        for i, chunk in enumerate(swapped(part, 16)):
            a2s[8 * half + i] = chunk.astype(BF)
    pl.semaphore_wait(barrier, 30)

    def a_exchange(d, src, dst, ss, rs):
        peer = in_fq(d)
        return remote(src.at[peer[2]], dst.at[fq], ss.at[d], rs.at[d], peer)

    def a_arrival(d, dst, ss, rs):
        peer = in_fq(-d)
        return remote(dst.at[peer[2]], dst.at[peer[2]], ss.at[d], rs.at[d], peer)

    for d in range(1, 16):
        a_exchange(d, a2s, a2r, as_sem, ar_sem).start()
    a2r[fq] = a2s[fq]

    loads[3].wait()
    classes = map_ref[...]
    kappa = jnp.zeros(classes.shape, F32)
    for c in range(8):
        kappa = jnp.where(classes == c, kap_ref[c], kappa)
    scale = 1.0 / (1.0 + 4.0 * kappa)
    ratio = scale * kappa
    mine[...] = jnp.concatenate([ratio, jnp.zeros((16, 96), F32)], axis=1)
    for x in range(32):
        inv[x] = jnp.broadcast_to(scale[:, x : x + 1], (16, 128))

    around = ((-1, 0), (1, 0), (0, -1), (0, 1), (-1, -1), (1, 1), (-1, 1), (1, -1))

    def there_is(i):
        dz, dx = around[i]
        return (sx + dz >= 0) & (sx + dz < G) & (sy + dx >= 0) & (sy + dx < G)

    def tile_at(i):
        dz, dx = around[i]
        return (add(sx, dz, G), add(sy, dx, G), fq)

    def m_copy(i):
        return remote(mine, near.at[i ^ 1], ms.at[i], mr.at[i ^ 1], tile_at(i))

    def m_in(i):
        return remote(near.at[i], near.at[i], ms.at[i], mr.at[i], tile_at(i))

    for i in range(8):
        @pl.when(there_is(i))
        def _():
            m_copy(i).start()

        @pl.when(jnp.logical_not(there_is(i)))
        def _():
            near[i] = jnp.zeros((16, 128), F32)

    @pl.loop(0, NF)
    def _(f):
        b0[f] = jnp.zeros((2, ROWS, 128), F32)

    for f in range(NF):
        a_copy(f).wait()
    for d in range(1, 16):
        a_arrival(d, a2r, as_sem, ar_sem).wait_recv()
    for i, block in enumerate(swapped([a2r[kb].astype(F32) for kb in range(16)], 1)):
        q[i // 2, sx, sy, i % 2] = block.astype(BF)

    def order_of(freqs):
        def pick(f, straight, other):
            turned = sum(((f == t).astype(jnp.int32) for t in freqs), jnp.int32(0))
            return straight + turned * (other - straight)

        def along(f, d, second):
            on_sx = pick(f, 0, d) if second else pick(f, d, 0)
            return (add(sx, on_sx, G), add(sy, d - on_sx, G), fq)

        def ones(f, d):
            return add(pick(f, sx, sy), d, G)

        def twos(f, d):
            return add(pick(f, sy, sx), d, G)

        return pick, along, ones, twos

    pick, along, ones, twos = order_of(GATHER_TURNED)
    s_pick, s_along, s_ones, s_twos = order_of(SUM_TURNED)

    def block_at(f, one, two):
        return q.at[f, pick(f, one, two), pick(f, two, one)]

    def g_copy(f, block, send, recv, d, second):
        return remote(block, block, send, recv, along(f, d, second))

    def z_own(f, side):
        return g_copy(f, q.at[f, sx, sy], zs.at[f, side], zr.at[f, side], 1 + 2 * side, False)

    def z_in(f, side):
        block = block_at(f, ones(f, 3 + 2 * side), twos(f, 0))
        return g_copy(f, block, zs.at[f, side], zr.at[f, side], 1, False)

    def z_across(f):
        return g_copy(f, q.at[f, sx, sy], zs.at[f, 2], zr.at[f, 2], 2, False)

    def z_far(f):
        block = block_at(f, ones(f, 2), twos(f, 0))
        return g_copy(f, block, zs.at[f, 2], zr.at[f, 2], 2, False)

    def x_own(f, row, side):
        block = block_at(f, row, twos(f, 0))
        return g_copy(f, block, xs.at[f, side, row], xr.at[f, side, row], 1 + 2 * side, True)

    def x_relay(f, row):
        side = lax.rem(f, 2)
        block = block_at(f, row, twos(f, 3 + 2 * side))
        return g_copy(f, block, xs.at[f, 2, row], xr.at[f, 2, row], 1 + 2 * side, True)

    def x_in(f, row, side):
        block = block_at(f, row, twos(f, 3 + 2 * side))
        return g_copy(f, block, xs.at[f, side, row], xr.at[f, side, row], 1, True)

    def x_far(f, row):
        block = block_at(f, row, twos(f, 2))
        return g_copy(f, block, xs.at[f, 2, row], xr.at[f, 2, row], 1, True)

    def h_bufs(i):
        return (hxs, hxr, i) if i < 2 else (hys, hyr, i - 2) if i < 4 else (hcs, hcr, i - 4)

    def h_out(f, i):
        s, r, k = h_bufs(i)
        return remote(s.at[f, k], r.at[f, k ^ 1], hs.at[f, i], hr.at[f, i ^ 1], tile_at(i))

    def h_in(f, i):
        _, r, k = h_bufs(i)
        return remote(r.at[f, k], r.at[f, k], hs.at[f, i], hr.at[f, i], tile_at(i))

    def corner(i, inside):
        dz, dx = around[i]
        x0 = (0 if dz < 0 else 30) if inside else (-2 if dz < 0 else 32)
        y0 = (0 if dx < 0 else 14) if inside else (-2 if dx < 0 else 16)
        return [(4 * c + 2 * m + n, c, row_at(x0 + m, y0 + n)) for c in range(2) for m in range(2) for n in range(2)]

    def send_edges(f):
        for c in range(2):
            for m in range(DEEP):
                hxs[f, 0, c, m] = b0[f, c, pl.ds(row_at(m, 0), 16), :].astype(BF)
                hxs[f, 1, c, m] = b0[f, c, pl.ds(row_at(32 - DEEP + m, 0), 16), :].astype(BF)
                hys[f, 0, c, m] = b0[f, c, pl.ds(row_at(0, m), 32, stride=PITCH), :].astype(BF)
                hys[f, 1, c, m] = b0[f, c, pl.ds(row_at(0, 16 - DEEP + m), 32, stride=PITCH), :].astype(BF)
        for i in range(4, 8):
            for to, c, at_row in corner(i, True):
                hcs[f, i - 4, to : to + 1, :] = b0[f, c, at_row : at_row + 1, :]
        for i in range(8):
            @pl.when(there_is(i))
            def _():
                h_out(f, i).start()

    def take_halos(f):
        for i in range(8):
            @pl.when(there_is(i))
            def _():
                h_in(f, i).wait_recv()
                for c in range(2):
                    for m in range(DEEP):
                        if i < 2:
                            x = m + (-DEEP, 32)[i]
                            b0[f, c, pl.ds(row_at(x, 0), 16), :] = hxr[f, i, c, m].astype(F32)
                        elif i < 4:
                            y = m + (-DEEP, 16)[i - 2]
                            b0[f, c, pl.ds(row_at(0, y), 32, stride=PITCH), :] = hyr[f, i - 2, c, m].astype(F32)
                if i >= 4:
                    for at, c, at_row in corner(i, False):
                        b0[f, c, at_row : at_row + 1, :] = hcr[f, i - 4, at : at + 1, :]

    def adjoint(f):
        real = q[f, :, :, 0].reshape(512, 128)
        imag = q[f, :, :, 1].reshape(512, 128)
        acc = jnp.dot(a[f, 0], jnp.concatenate([real, imag], axis=1), preferred_element_type=F32)
        acc += jnp.dot(a[f, 1], jnp.concatenate([imag, -real], axis=1), preferred_element_type=F32)
        for x in range(32):
            for c in range(2):
                b0[f, c, pl.ds(row_at(x, 0), 16), :] = (
                    acc[16 * x : 16 * x + 16, 128 * c : 128 * c + 128] * inv[x]
                )
        send_edges(f)

    @pl.loop(0, NF)
    def _(f):
        for side in range(2):
            z_own(f, side).start()
        z_across(f).start()
        for side in range(2):
            x_own(f, ones(f, 0), side).start()

    for i in range(8):
        @pl.when(there_is(i))
        def _():
            m_in(i).wait_recv()
    maps = {d: near[i] for i, d in enumerate(around)}
    maps[0, 0] = mine[...]
    line = lax.broadcasted_iota(jnp.int32, (8, 128), 0)

    def cells(x, dx, rows):
        dz = -1 if x < 0 else 1 if x > 31 else 0
        x -= 32 * dz
        return jnp.broadcast_to(maps[dz, dx][rows, x : x + 1], (rows.stop - rows.start, 128))

    for x in range(-DEEP, 32 + DEEP):
        kd[pl.ds(row_at(x, 0), 16), :] = cells(x, 0, slice(0, 16))
        rim = jnp.where(line < DEEP, cells(x, 1, slice(0, 8)), 0.0)
        if x < 31 + DEEP:
            rim = jnp.where(line >= 8 - DEEP, cells(x + 1, -1, slice(8, 16)), rim)
        kd[pl.ds(row_at(x, 16), 8), :] = rim
    for start in (0, ROWS - PITCH):
        kd[pl.ds(start, PITCH), :] = jnp.zeros((PITCH, 128), F32)
    kd[pl.ds(16, 8), :] = jnp.where(line >= 8 - DEEP, cells(-DEEP, -1, slice(8, 16)), 0.0)

    def pass_on(f, row):
        x_in(f, row, lax.rem(f, 2)).wait_recv()
        x_relay(f, row).start()

    def row_of(f, side):
        return ones(f, 3 + 2 * side)

    def swept(f, c, start, size, p):
        beside = (
            p[c, pl.ds(start - PITCH, size), :] + p[c, pl.ds(start + PITCH, size), :]
            + p[c, pl.ds(start - 1, size), :] + p[c, pl.ds(start + 1, size), :]
        )
        return b0[f, c, pl.ds(start, size), :] + kd[pl.ds(start, size), :] * beside

    def sweep(f, before, after, layers):
        low = row_at(-layers, -layers) // 8 * 8
        high = -(-row_at(31 + layers, 16 + layers) // 8) * 8
        for start in range(low, high, 16):
            size = min(16, high - start)
            for c in range(2):
                after[c, pl.ds(start, size), :] = swept(f, c, start, size, before)

    def forward(f):
        take_halos(f)
        sweep(f, b0.at[f], p1, 2)
        sweep(f, p1, p2, 1)
        for x in range(32):
            for c in range(2):
                fh[c, pl.ds(16 * x, 16), :] = swept(f, c, row_at(x, 0), 16, p2).astype(BF)
        real, imag = fh[0], fh[1]
        acc = jnp.dot(at[f, 0], jnp.concatenate([real, imag], axis=1), preferred_element_type=F32)
        acc += jnp.dot(at[f, 1], jnp.concatenate([-imag, real], axis=1), preferred_element_type=F32)
        for t in range(16):
            for c in range(2):
                there = s_pick(f, t % G, t // G)
                row = lax.rem(s_pick(f, t // G, t % G) + G - s_ones(f, 0), G)
                out[f, there, row, c] = acc[32 * t : 32 * t + 32, 128 * c : 128 * c + 128].astype(BF)

    def way(f):
        return 1 + 2 * lax.rem(f, 2)

    def back(f):
        return 3 - 2 * lax.rem(f, 2)

    rest = (pl.ds(1, G - 1), pl.ds(0, 1))

    def x_sum(f, kind, part):
        d, to, land = ((2, way(f), rxf), (back(f), back(f), rxd), (way(f), way(f), rxc))[kind]
        return remote(
            out.at[f, s_twos(f, d), rest[part]], land.at[f, rest[part]],
            rxs.at[f, kind, part], rxr.at[f, kind, part], s_along(f, to, True),
        )

    def z_sum(f, d):
        return remote(sx_buf.at[f, d], rz.at[f, d], rzs.at[f, d], rzr.at[f, d], s_along(f, d, False))

    def x_relay_sum(f, part):
        x_sum(f, 0, part).wait_recv()
        there, rows = s_twos(f, way(f)), rest[part]
        out[f, there, rows] = (out[f, there, rows].astype(F32) + rxf[f, rows].astype(F32)).astype(BF)
        x_sum(f, 2, part).start()

    def x_total(f, part):
        x_sum(f, 1, part).wait_recv()
        x_sum(f, 2, part).wait_recv()
        rows = rest[part]
        return out[f, s_twos(f, 0), rows].astype(F32) + rxd[f, rows].astype(F32) + rxc[f, rows].astype(F32)

    @pl.loop(0, NF + X_TOTAL)
    def _(i):
        def stage(first):
            return pl.when((i >= first) & (i < first + NF))

        @stage(0)
        def _():
            first = lax.rem(i, 2)
            z_in(i, first).wait_recv()
            for side in range(2):
                x_own(i, row_of(i, first), side).start()
            z_in(i, 1 - first).wait_recv()
            for side in range(2):
                x_own(i, row_of(i, 1 - first), side).start()

        @stage(FAR)
        def _():
            f = i - FAR
            pass_on(f, ones(f, 0))
            z_far(f).wait_recv()
            for side in range(2):
                x_own(f, ones(f, 2), side).start()

        @stage(PASS)
        def _():
            f = i - PASS
            first = lax.rem(f, 2)
            pass_on(f, row_of(f, first))
            pass_on(f, row_of(f, 1 - first))

        @stage(PASS_FAR)
        def _():
            f = i - PASS_FAR
            pass_on(f, ones(f, 2))

        @stage(0)
        def _():
            for c in range(2):
                at[i, c] = a[i, c].T

        @stage(ADJOINT)
        def _():
            f = i - ADJOINT
            for row in range(G):
                x_in(f, row, 1 - lax.rem(f, 2)).wait_recv()
                x_far(f, row).wait_recv()
            adjoint(f)

        @stage(FORWARD)
        def _():
            f = i - FORWARD
            forward(f)
            x_sum(f, 0, 0).start()
            x_sum(f, 1, 0).start()

        @stage(X_RELAY)
        def _():
            x_relay_sum(i - X_RELAY, 0)

        @pl.when(i == OWN_ROW)
        def _():
            @pl.loop(0, NF)
            def _(f):
                x_sum(f, 0, 1).start()
                x_sum(f, 1, 1).start()

        @stage(X_TOTAL)
        def _():
            f = i - X_TOTAL
            sx_buf[f, rest[0]] = x_total(f, 0).astype(BF)
            for d in range(1, G):
                z_sum(f, d).start()

        @pl.when(i == OWN_RELAY)
        def _():
            @pl.loop(0, NF)
            def _(f):
                x_relay_sum(f, 1)

    @pl.loop(0, NF)
    def _(f):
        total = x_total(f, 1)[0]
        for d in range(1, G):
            z_sum(f, d).wait_recv()
            total += rz[f, d].astype(F32)
        fin[f] = total

    for kb, chunk in enumerate(swapped([fin[i // 2, i % 2] for i in range(16)], 1)):
        r2s[kb] = chunk.astype(BF)
    for d in range(1, 16):
        a_exchange(d, r2s, r2r, bs_sem, br_sem).start()
    r2r[fq] = r2s[fq]
    for d in range(1, 16):
        a_arrival(d, r2r, bs_sem, br_sem).wait_recv()
    for load in loads[4:]:
        load.wait()
    halves = []
    for half in range(2):
        part = swapped([r2r[8 * half + i].astype(F32) for i in range(8)], 16)
        halves.append(jnp.concatenate(part, axis=0))
    returned = jnp.dot(
        jnp.concatenate(halves, axis=1), back_ref[...], preferred_element_type=F32, precision=HIGHEST
    )

    for k in range(8):
        less = step_ref[k] * (dir_ref[k] + noise_ref[...] * returned[32 * k : 32 * k + 32])
        delta[k] = less
        new = res_ref[k] - less
        total = jnp.sum(jnp.sum(new * new, axis=1, keepdims=True), axis=0, keepdims=True)
        ns[k : k + 1, :] = jnp.broadcast_to(total, (1, 128))
    leave = pltpu.make_async_copy(delta, delta_hbm, out_sem)

    def n_copy(d):
        return remote(ns, nr.at[d], ns_sem.at[d], nr_sem.at[d], in_tiles(d))

    for d in range(1, 16):
        n_copy(d).start()
    leave.start()

    for d in range(1, 16):
        a_exchange(d, a2s, a2r, as_sem, ar_sem).wait_send()
        a_exchange(d, r2s, r2r, bs_sem, br_sem).wait_send()

    @pl.loop(0, NF)
    def _(f):
        for side in range(2):
            z_own(f, side).wait_send()
            for row in range(G):
                x_own(f, row, side).wait_send()
        z_across(f).wait_send()
        for row in range(G):
            x_relay(f, row).wait_send()
        for d in range(1, G):
            z_sum(f, d).wait_send()
        for kind in range(3):
            for part in range(2):
                x_sum(f, kind, part).wait_send()
        for i in range(8):
            @pl.when(there_is(i))
            def _():
                h_out(f, i).wait_send()

    for i in range(8):
        @pl.when(there_is(i))
        def _():
            m_copy(i).wait_send()

    norm = ns[...]
    for d in range(1, 16):
        n_copy(d).wait_recv()
        norm += nr[d]
    column = lax.broadcasted_iota(jnp.int32, (8, 128), 0)
    old = jnp.ones((8, 128), F32)
    for k in range(8):
        old = jnp.where(column == k, old_ref[k], old)
    growth = norm / old
    for k in range(8):
        norm_ref[k] = norm[k, 0]
        ratio_ref[k] = growth[k, 0]
    leave.wait()
    for d in range(1, 16):
        n_copy(d).wait_send()


def on_device(
    spectra, noise_weight, class_map, class_kappa, solution, residual, direction, step_length, old_norm
):
    forward_table, back_table = tables(128, 256, NF)
    smem = pl.BlockSpec(memory_space=pltpu.SMEM)
    dma = pltpu.SemaphoreType.DMA
    field = pltpu.VMEM((2, ROWS, 128), F32)
    chunks = pltpu.VMEM((16, 32, 128), BF)
    x_part = pltpu.VMEM((NF, G, 2, 32, 128), BF)
    hbm = pl.BlockSpec(memory_space=pl.ANY)
    delta, norm, growth = pl.pallas_call(
        kernel,
        out_shape=(
            jax.ShapeDtypeStruct(residual.shape, F32),
            jax.ShapeDtypeStruct((8,), F32),
            jax.ShapeDtypeStruct((8,), F32),
        ),
        in_specs=[hbm] * 6 + [smem] * 3 + [hbm],
        out_specs=(hbm, smem, smem),
        scratch_shapes=[
            pltpu.VMEM(direction.shape, F32), pltpu.VMEM((32, 256), F32), pltpu.VMEM((256, 256), F32),
            pltpu.VMEM((16, 32), jnp.int32), pltpu.VMEM((256, 256), F32), pltpu.VMEM(direction.shape, F32),
            pltpu.VMEM(direction.shape, F32), dma((6,)), dma,
            pltpu.VMEM((NF, 2, 512, 512), BF),
            pltpu.VMEM((NF, 2, 512, 512), BF),
            pltpu.VMEM((NF, G, G, 2, 32, 128), BF),
            pltpu.VMEM((NF, 2, ROWS, 128), F32), field, field,
            pltpu.VMEM((ROWS, 128), F32), pltpu.VMEM((32, 16, 128), F32),
            pltpu.VMEM((NF, G, G, 2, 32, 128), BF),
            x_part,
            pltpu.VMEM((NF, 2, 32, 128), F32),
            chunks, chunks, chunks, chunks,
            pltpu.VMEM((NF, 2, 2, DEEP, 16, 128), BF), pltpu.VMEM((NF, 2, 2, DEEP, 16, 128), BF),
            pltpu.VMEM((NF, 2, 2, DEEP, 32, 128), BF), pltpu.VMEM((NF, 2, 2, DEEP, 32, 128), BF),
            pltpu.VMEM((NF, 4, 8, 128), F32), pltpu.VMEM((NF, 4, 8, 128), F32),
            pltpu.VMEM((16, 128), F32), pltpu.VMEM((8, 16, 128), F32),
            x_part, x_part, x_part, x_part,
            pltpu.VMEM((8, 128), F32), pltpu.VMEM((16, 8, 128), F32),
            pltpu.VMEM((2, 512, 128), BF),
            dma((NF,)),
            dma((16,)), dma((16,)), dma((16,)), dma((16,)), dma((16,)), dma((16,)),
            dma((NF, 3)), dma((NF, 3)), dma((NF, 3, G)), dma((NF, 3, G)),
            dma((NF, 8)), dma((NF, 8)), dma((8,)), dma((8,)),
            dma((NF, 3, 2)), dma((NF, 3, 2)), dma((NF, G)), dma((NF, G)),
        ],
        compiler_params=pltpu.CompilerParams(
            collective_id=0, has_side_effects=True, vmem_limit_bytes=62 * 1024 * 1024
        ),
        name="hessian_step",
    )(
        direction, noise_weight, jnp.asarray(forward_table), class_map.T, jnp.asarray(back_table), residual,
        class_kappa, step_length, old_norm, spectra.reshape(NF, 2, 512, 512),
    )
    new_residual = residual - delta
    new_norm = jnp.maximum(norm, 0.0)
    new_solution = solution + step_length[:, None, None] * direction
    new_direction = new_residual + growth[:, None, None] * direction
    return (new_solution, new_residual, new_direction, new_norm)


def solution(mesh):
    columns = P("fq", ("sx", "sy"), None)
    return jax.shard_map(
        on_device,
        mesh=mesh,
        in_specs=(
            P("fq", None, "sx", "sy", None), P(("sx", "sy"), None), P("sx", "sy"), P(),
            columns, columns, columns, P("fq"), P("fq"),
        ),
        out_specs=(columns, columns, columns, P("fq")),
        check_vma=False,
    )
```

```python
import functools
import math

import jax
import jax.numpy as jnp
import numpy as np
from jax import lax
from jax.experimental import pallas as pl
from jax.experimental.pallas import tpu as pltpu
from jax.sharding import PartitionSpec as P

MESH = pl.DeviceIdType.MESH
HIGHEST = lax.Precision.HIGHEST
BF, F32 = jnp.bfloat16, jnp.float32
PITCH = 24
NF = 8
G = 4
GATHER_TURNED, SUM_TURNED = (3,), (0, 3)
FAR, PASS, PASS_FAR, ADJOINT, FORWARD, X_RELAY, X_TOTAL = 1, 2, 4, 6, 9, 12, 15
OWN_ROW, OWN_RELAY = NF + X_RELAY - 1, NF + X_TOTAL - 1
DEEP = 3
ROWS = PITCH * (32 + 2 * DEEP + 2)


def tables(freq_count, time_steps, per_block):
    freq = np.arange(freq_count)
    phase = (freq[:, None] * np.arange(time_steps)[None, :] % time_steps) * (2.0 * math.pi / time_steps)
    factor = 1.0 / math.sqrt(time_steps)
    both = np.stack([np.cos(phase), -np.sin(phase)], axis=1) * factor
    doubled = both * np.where(freq == 0, 1.0, 2.0)[:, None, None]
    forward = both.reshape(2 * freq_count, time_steps).T
    back = doubled.reshape(2 * freq_count, time_steps)
    return forward.astype(np.float32), back.astype(np.float32)


def swapped(arrays, unit):
    arrays = list(arrays)
    lane = lax.broadcasted_iota(jnp.int32, arrays[0].shape, 1)
    bit = 1
    while bit < len(arrays):
        here = ((lane // unit) & bit) != 0
        for i in range(len(arrays)):
            if i & bit == 0:
                a, c = arrays[i], arrays[i | bit]
                arrays[i] = jnp.where(here, pltpu.roll(c, bit * unit, 1), a)
                arrays[i | bit] = jnp.where(here, c, pltpu.roll(a, 128 - bit * unit, 1))
        bit *= 2
    return arrays


def row_at(x, y):
    return PITCH * (x + DEEP + 1) + y


def remote(src, dst, send, recv, device):
    return pltpu.make_async_remote_copy(
        src_ref=src, dst_ref=dst, send_sem=send, recv_sem=recv, device_id=device, device_id_type=MESH
    )


def kernel(
    dir_hbm, noise_hbm, fwd_hbm, map_hbm, back_hbm, res_hbm, kap_ref, step_ref, old_ref, spectra_ref,
    delta_hbm, norm_ref, ratio_ref,
    dir_ref, noise_ref, fwd_ref, map_ref, back_ref, res_ref, delta, in_sem, out_sem,
    a, at, q, b0, p1, p2, kd, inv, out, sx_buf, fin, a2s, a2r, r2s, r2r,
    hxs, hxr, hys, hyr, hcs, hcr, mine, near, rxf, rxd, rxc, rz, ns, nr, fh,
    a_sem, as_sem, ar_sem, bs_sem, br_sem, ns_sem, nr_sem,
    zs, zr, xs, xr, hs, hr, ms, mr, rxs, rxr, rzs, rzr,
):
    sx, sy, fq = lax.axis_index("sx"), lax.axis_index("sy"), lax.axis_index("fq")
    tile = sx * G + sy

    def add(i, d, n):
        return lax.rem(i + d + n, n)

    def on_z(d):
        return (add(sx, d, G), sy, fq)

    def on_x(d):
        return (sx, add(sy, d, G), fq)

    def in_fq(d):
        return (sx, sy, add(fq, d, 16))

    def in_tiles(d):
        other = add(tile, d, 16)
        return (other // G, lax.rem(other, G), fq)

    barrier = pltpu.get_barrier_semaphore()
    for d in range(1, 16):
        pl.semaphore_signal(barrier, inc=1, device_id=in_fq(d), device_id_type=MESH)
        pl.semaphore_signal(barrier, inc=1, device_id=in_tiles(d), device_id_type=MESH)

    loads = [
        pltpu.make_async_copy(src, dst, in_sem.at[i])
        for i, (src, dst) in enumerate((
            (dir_hbm, dir_ref), (noise_hbm, noise_ref), (fwd_hbm, fwd_ref),
            (map_hbm, map_ref), (back_hbm, back_ref), (res_hbm, res_ref),
        ))
    ]
    for load in loads[:3]:
        load.start()

    def a_copy(f):
        return pltpu.make_async_copy(spectra_ref.at[f], a.at[f], a_sem.at[f])

    for load in loads[:3]:
        load.wait()
    for load in loads[3:]:
        load.start()
    for f in range(NF):
        a_copy(f).start()

    weighted = (dir_ref[...] * noise_ref[...][None]).reshape(256, 256)
    spec = jnp.dot(weighted, fwd_ref[...], preferred_element_type=F32, precision=HIGHEST)
    for half in range(2):
        part = [spec[32 * k : 32 * k + 32, 128 * half : 128 * half + 128] for k in range(8)]
        for i, chunk in enumerate(swapped(part, 16)):
            a2s[8 * half + i] = chunk.astype(BF)
    pl.semaphore_wait(barrier, 30)

    def a_exchange(d, src, dst, ss, rs):
        peer = in_fq(d)
        return remote(src.at[peer[2]], dst.at[fq], ss.at[d], rs.at[d], peer)

    def a_arrival(d, dst, ss, rs):
        peer = in_fq(-d)
        return remote(dst.at[peer[2]], dst.at[peer[2]], ss.at[d], rs.at[d], peer)

    for d in range(1, 16):
        a_exchange(d, a2s, a2r, as_sem, ar_sem).start()
    a2r[fq] = a2s[fq]

    loads[3].wait()
    classes = map_ref[...]
    kappa = jnp.zeros(classes.shape, F32)
    for c in range(8):
        kappa = jnp.where(classes == c, kap_ref[c], kappa)
    scale = 1.0 / (1.0 + 4.0 * kappa)
    ratio = scale * kappa
    mine[...] = jnp.concatenate([ratio, jnp.zeros((16, 96), F32)], axis=1)
    for x in range(32):
        inv[x] = jnp.broadcast_to(scale[:, x : x + 1], (16, 128))

    around = ((-1, 0), (1, 0), (0, -1), (0, 1), (-1, -1), (1, 1), (-1, 1), (1, -1))

    def there_is(i):
        dz, dx = around[i]
        return (sx + dz >= 0) & (sx + dz < G) & (sy + dx >= 0) & (sy + dx < G)

    def tile_at(i):
        dz, dx = around[i]
        return (add(sx, dz, G), add(sy, dx, G), fq)

    def m_copy(i):
        return remote(mine, near.at[i ^ 1], ms.at[i], mr.at[i ^ 1], tile_at(i))

    def m_in(i):
        return remote(near.at[i], near.at[i], ms.at[i], mr.at[i], tile_at(i))

    for i in range(8):
        @pl.when(there_is(i))
        def _():
            m_copy(i).start()

        @pl.when(jnp.logical_not(there_is(i)))
        def _():
            near[i] = jnp.zeros((16, 128), F32)

    @pl.loop(0, NF)
    def _(f):
        b0[f] = jnp.zeros((2, ROWS, 128), F32)

    for f in range(NF):
        a_copy(f).wait()
    for d in range(1, 16):
        a_arrival(d, a2r, as_sem, ar_sem).wait_recv()
    for i, block in enumerate(swapped([a2r[kb].astype(F32) for kb in range(16)], 1)):
        q[i // 2, sx, sy, i % 2] = block.astype(BF)

    def order_of(freqs):
        def pick(f, straight, other):
            turned = sum(((f == t).astype(jnp.int32) for t in freqs), jnp.int32(0))
            return straight + turned * (other - straight)

        def along(f, d, second):
            on_sx = pick(f, 0, d) if second else pick(f, d, 0)
            return (add(sx, on_sx, G), add(sy, d - on_sx, G), fq)

        def ones(f, d):
            return add(pick(f, sx, sy), d, G)

        def twos(f, d):
            return add(pick(f, sy, sx), d, G)

        return pick, along, ones, twos

    pick, along, ones, twos = order_of(GATHER_TURNED)
    s_pick, s_along, s_ones, s_twos = order_of(SUM_TURNED)

    def block_at(f, one, two):
        return q.at[f, pick(f, one, two), pick(f, two, one)]

    def g_copy(f, block, send, recv, d, second):
        return remote(block, block, send, recv, along(f, d, second))

    def z_own(f, side):
        return g_copy(f, q.at[f, sx, sy], zs.at[f, side], zr.at[f, side], 1 + 2 * side, False)

    def z_in(f, side):
        block = block_at(f, ones(f, 3 + 2 * side), twos(f, 0))
        return g_copy(f, block, zs.at[f, side], zr.at[f, side], 1, False)

    def z_across(f):
        return g_copy(f, q.at[f, sx, sy], zs.at[f, 2], zr.at[f, 2], 2, False)

    def z_far(f):
        block = block_at(f, ones(f, 2), twos(f, 0))
        return g_copy(f, block, zs.at[f, 2], zr.at[f, 2], 2, False)

    def x_own(f, row, side):
        block = block_at(f, row, twos(f, 0))
        return g_copy(f, block, xs.at[f, side, row], xr.at[f, side, row], 1 + 2 * side, True)

    def x_relay(f, row):
        side = lax.rem(f, 2)
        block = block_at(f, row, twos(f, 3 + 2 * side))
        return g_copy(f, block, xs.at[f, 2, row], xr.at[f, 2, row], 1 + 2 * side, True)

    def x_in(f, row, side):
        block = block_at(f, row, twos(f, 3 + 2 * side))
        return g_copy(f, block, xs.at[f, side, row], xr.at[f, side, row], 1, True)

    def x_far(f, row):
        block = block_at(f, row, twos(f, 2))
        return g_copy(f, block, xs.at[f, 2, row], xr.at[f, 2, row], 1, True)

    def h_bufs(i):
        return (hxs, hxr, i) if i < 2 else (hys, hyr, i - 2) if i < 4 else (hcs, hcr, i - 4)

    def h_out(f, i):
        s, r, k = h_bufs(i)
        return remote(s.at[f, k], r.at[f, k ^ 1], hs.at[f, i], hr.at[f, i ^ 1], tile_at(i))

    def h_in(f, i):
        _, r, k = h_bufs(i)
        return remote(r.at[f, k], r.at[f, k], hs.at[f, i], hr.at[f, i], tile_at(i))

    def corner(i, inside):
        dz, dx = around[i]
        x0 = (0 if dz < 0 else 30) if inside else (-2 if dz < 0 else 32)
        y0 = (0 if dx < 0 else 14) if inside else (-2 if dx < 0 else 16)
        return [(4 * c + 2 * m + n, c, row_at(x0 + m, y0 + n)) for c in range(2) for m in range(2) for n in range(2)]

    def send_edges(f):
        for c in range(2):
            for m in range(DEEP):
                hxs[f, 0, c, m] = b0[f, c, pl.ds(row_at(m, 0), 16), :].astype(BF)
                hxs[f, 1, c, m] = b0[f, c, pl.ds(row_at(32 - DEEP + m, 0), 16), :].astype(BF)
                hys[f, 0, c, m] = b0[f, c, pl.ds(row_at(0, m), 32, stride=PITCH), :].astype(BF)
                hys[f, 1, c, m] = b0[f, c, pl.ds(row_at(0, 16 - DEEP + m), 32, stride=PITCH), :].astype(BF)
        for i in range(4, 8):
            for to, c, at_row in corner(i, True):
                hcs[f, i - 4, to : to + 1, :] = b0[f, c, at_row : at_row + 1, :]
        for i in range(8):
            @pl.when(there_is(i))
            def _():
                h_out(f, i).start()

    def take_halos(f):
        for i in range(8):
            @pl.when(there_is(i))
            def _():
                h_in(f, i).wait_recv()
                for c in range(2):
                    for m in range(DEEP):
                        if i < 2:
                            x = m + (-DEEP, 32)[i]
                            b0[f, c, pl.ds(row_at(x, 0), 16), :] = hxr[f, i, c, m].astype(F32)
                        elif i < 4:
                            y = m + (-DEEP, 16)[i - 2]
                            b0[f, c, pl.ds(row_at(0, y), 32, stride=PITCH), :] = hyr[f, i - 2, c, m].astype(F32)
                if i >= 4:
                    for at, c, at_row in corner(i, False):
                        b0[f, c, at_row : at_row + 1, :] = hcr[f, i - 4, at : at + 1, :]

    def adjoint(f):
        real = q[f, :, :, 0].reshape(512, 128)
        imag = q[f, :, :, 1].reshape(512, 128)
        acc = jnp.dot(a[f, 0], jnp.concatenate([real, imag], axis=1), preferred_element_type=F32)
        acc += jnp.dot(a[f, 1], jnp.concatenate([imag, -real], axis=1), preferred_element_type=F32)
        for x in range(32):
            for c in range(2):
                b0[f, c, pl.ds(row_at(x, 0), 16), :] = (
                    acc[16 * x : 16 * x + 16, 128 * c : 128 * c + 128] * inv[x]
                )
        send_edges(f)

    @pl.loop(0, NF)
    def _(f):
        for side in range(2):
            z_own(f, side).start()
        z_across(f).start()
        for side in range(2):
            x_own(f, ones(f, 0), side).start()

    for i in range(8):
        @pl.when(there_is(i))
        def _():
            m_in(i).wait_recv()
    maps = {d: near[i] for i, d in enumerate(around)}
    maps[0, 0] = mine[...]
    line = lax.broadcasted_iota(jnp.int32, (8, 128), 0)

    def cells(x, dx, rows):
        dz = -1 if x < 0 else 1 if x > 31 else 0
        x -= 32 * dz
        return jnp.broadcast_to(maps[dz, dx][rows, x : x + 1], (rows.stop - rows.start, 128))

    for x in range(-DEEP, 32 + DEEP):
        kd[pl.ds(row_at(x, 0), 16), :] = cells(x, 0, slice(0, 16))
        rim = jnp.where(line < DEEP, cells(x, 1, slice(0, 8)), 0.0)
        if x < 31 + DEEP:
            rim = jnp.where(line >= 8 - DEEP, cells(x + 1, -1, slice(8, 16)), rim)
        kd[pl.ds(row_at(x, 16), 8), :] = rim
    for start in (0, ROWS - PITCH):
        kd[pl.ds(start, PITCH), :] = jnp.zeros((PITCH, 128), F32)
    kd[pl.ds(16, 8), :] = jnp.where(line >= 8 - DEEP, cells(-DEEP, -1, slice(8, 16)), 0.0)

    def pass_on(f, row):
        x_in(f, row, lax.rem(f, 2)).wait_recv()
        x_relay(f, row).start()

    def row_of(f, side):
        return ones(f, 3 + 2 * side)

    def swept(f, c, start, size, p):
        beside = (
            p[c, pl.ds(start - PITCH, size), :] + p[c, pl.ds(start + PITCH, size), :]
            + p[c, pl.ds(start - 1, size), :] + p[c, pl.ds(start + 1, size), :]
        )
        return b0[f, c, pl.ds(start, size), :] + kd[pl.ds(start, size), :] * beside

    def sweep(f, before, after, layers):
        low = row_at(-layers, -layers) // 8 * 8
        high = -(-row_at(31 + layers, 16 + layers) // 8) * 8
        for start in range(low, high, 16):
            size = min(16, high - start)
            for c in range(2):
                after[c, pl.ds(start, size), :] = swept(f, c, start, size, before)

    def forward(f):
        take_halos(f)
        sweep(f, b0.at[f], p1, 2)
        sweep(f, p1, p2, 1)
        for x in range(32):
            for c in range(2):
                fh[c, pl.ds(16 * x, 16), :] = swept(f, c, row_at(x, 0), 16, p2).astype(BF)
        real, imag = fh[0], fh[1]
        acc = jnp.dot(at[f, 0], jnp.concatenate([real, imag], axis=1), preferred_element_type=F32)
        acc += jnp.dot(at[f, 1], jnp.concatenate([-imag, real], axis=1), preferred_element_type=F32)
        for t in range(16):
            for c in range(2):
                there = s_pick(f, t % G, t // G)
                row = lax.rem(s_pick(f, t // G, t % G) + G - s_ones(f, 0), G)
                out[f, there, row, c] = acc[32 * t : 32 * t + 32, 128 * c : 128 * c + 128].astype(BF)

    def way(f):
        return 1 + 2 * lax.rem(f, 2)

    def back(f):
        return 3 - 2 * lax.rem(f, 2)

    rest = (pl.ds(1, G - 1), pl.ds(0, 1))

    def x_sum(f, kind, part):
        d, to, land = ((2, way(f), rxf), (back(f), back(f), rxd), (way(f), way(f), rxc))[kind]
        return remote(
            out.at[f, s_twos(f, d), rest[part]], land.at[f, rest[part]],
            rxs.at[f, kind, part], rxr.at[f, kind, part], s_along(f, to, True),
        )

    def z_sum(f, d):
        return remote(sx_buf.at[f, d], rz.at[f, d], rzs.at[f, d], rzr.at[f, d], s_along(f, d, False))

    def x_relay_sum(f, part):
        x_sum(f, 0, part).wait_recv()
        there, rows = s_twos(f, way(f)), rest[part]
        out[f, there, rows] = (out[f, there, rows].astype(F32) + rxf[f, rows].astype(F32)).astype(BF)
        x_sum(f, 2, part).start()

    def x_total(f, part):
        x_sum(f, 1, part).wait_recv()
        x_sum(f, 2, part).wait_recv()
        rows = rest[part]
        return out[f, s_twos(f, 0), rows].astype(F32) + rxd[f, rows].astype(F32) + rxc[f, rows].astype(F32)

    @pl.loop(0, NF + X_TOTAL)
    def _(i):
        def stage(first):
            return pl.when((i >= first) & (i < first + NF))

        @stage(0)
        def _():
            first = lax.rem(i, 2)
            z_in(i, first).wait_recv()
            for side in range(2):
                x_own(i, row_of(i, first), side).start()
            z_in(i, 1 - first).wait_recv()
            for side in range(2):
                x_own(i, row_of(i, 1 - first), side).start()

        @stage(FAR)
        def _():
            f = i - FAR
            pass_on(f, ones(f, 0))
            z_far(f).wait_recv()
            for side in range(2):
                x_own(f, ones(f, 2), side).start()

        @stage(PASS)
        def _():
            f = i - PASS
            first = lax.rem(f, 2)
            pass_on(f, row_of(f, first))
            pass_on(f, row_of(f, 1 - first))

        @stage(PASS_FAR)
        def _():
            f = i - PASS_FAR
            pass_on(f, ones(f, 2))

        @stage(0)
        def _():
            for c in range(2):
                at[i, c] = a[i, c].T

        @stage(ADJOINT)
        def _():
            f = i - ADJOINT
            for row in range(G):
                x_in(f, row, 1 - lax.rem(f, 2)).wait_recv()
                x_far(f, row).wait_recv()
            adjoint(f)

        @stage(FORWARD)
        def _():
            f = i - FORWARD
            forward(f)
            x_sum(f, 0, 0).start()
            x_sum(f, 1, 0).start()

        @stage(X_RELAY)
        def _():
            x_relay_sum(i - X_RELAY, 0)

        @pl.when(i == OWN_ROW)
        def _():
            @pl.loop(0, NF)
            def _(f):
                x_sum(f, 0, 1).start()
                x_sum(f, 1, 1).start()

        @stage(X_TOTAL)
        def _():
            f = i - X_TOTAL
            sx_buf[f, rest[0]] = x_total(f, 0).astype(BF)
            for d in range(1, G):
                z_sum(f, d).start()

        @pl.when(i == OWN_RELAY)
        def _():
            @pl.loop(0, NF)
            def _(f):
                x_relay_sum(f, 1)

    @pl.loop(0, NF)
    def _(f):
        total = x_total(f, 1)[0]
        for d in range(1, G):
            z_sum(f, d).wait_recv()
            total += rz[f, d].astype(F32)
        fin[f] = total

    for kb, chunk in enumerate(swapped([fin[i // 2, i % 2] for i in range(16)], 1)):
        r2s[kb] = chunk.astype(BF)
    for d in range(1, 16):
        a_exchange(d, r2s, r2r, bs_sem, br_sem).start()
    r2r[fq] = r2s[fq]
    for d in range(1, 16):
        a_arrival(d, r2r, bs_sem, br_sem).wait_recv()
    for load in loads[4:]:
        load.wait()
    halves = []
    for half in range(2):
        part = swapped([r2r[8 * half + i].astype(F32) for i in range(8)], 16)
        halves.append(jnp.concatenate(part, axis=0))
    returned = jnp.dot(
        jnp.concatenate(halves, axis=1), back_ref[...], preferred_element_type=F32, precision=HIGHEST
    )

    for k in range(8):
        less = step_ref[k] * (dir_ref[k] + noise_ref[...] * returned[32 * k : 32 * k + 32])
        delta[k] = less
        new = res_ref[k] - less
        total = jnp.sum(jnp.sum(new * new, axis=1, keepdims=True), axis=0, keepdims=True)
        ns[k : k + 1, :] = jnp.broadcast_to(total, (1, 128))
    leave = pltpu.make_async_copy(delta, delta_hbm, out_sem)

    def n_copy(d):
        return remote(ns, nr.at[d], ns_sem.at[d], nr_sem.at[d], in_tiles(d))

    for d in range(1, 16):
        n_copy(d).start()
    leave.start()

    for d in range(1, 16):
        a_exchange(d, a2s, a2r, as_sem, ar_sem).wait_send()
        a_exchange(d, r2s, r2r, bs_sem, br_sem).wait_send()

    @pl.loop(0, NF)
    def _(f):
        for side in range(2):
            z_own(f, side).wait_send()
            for row in range(G):
                x_own(f, row, side).wait_send()
        z_across(f).wait_send()
        for row in range(G):
            x_relay(f, row).wait_send()
        for d in range(1, G):
            z_sum(f, d).wait_send()
        for kind in range(3):
            for part in range(2):
                x_sum(f, kind, part).wait_send()
        for i in range(8):
            @pl.when(there_is(i))
            def _():
                h_out(f, i).wait_send()

    for i in range(8):
        @pl.when(there_is(i))
        def _():
            m_copy(i).wait_send()

    norm = ns[...]
    for d in range(1, 16):
        n_copy(d).wait_recv()
        norm += nr[d]
    column = lax.broadcasted_iota(jnp.int32, (8, 128), 0)
    old = jnp.ones((8, 128), F32)
    for k in range(8):
        old = jnp.where(column == k, old_ref[k], old)
    growth = norm / old
    for k in range(8):
        norm_ref[k] = norm[k, 0]
        ratio_ref[k] = growth[k, 0]
    leave.wait()
    for d in range(1, 16):
        n_copy(d).wait_send()


def on_device(
    spectra, noise_weight, class_map, class_kappa, solution, residual, direction, step_length, old_norm
):
    forward_table, back_table = tables(128, 256, NF)
    smem = pl.BlockSpec(memory_space=pltpu.SMEM)
    dma = pltpu.SemaphoreType.DMA
    field = pltpu.VMEM((2, ROWS, 128), F32)
    chunks = pltpu.VMEM((16, 32, 128), BF)
    x_part = pltpu.VMEM((NF, G, 2, 32, 128), BF)
    hbm = pl.BlockSpec(memory_space=pl.ANY)
    delta, norm, growth = pl.pallas_call(
        kernel,
        out_shape=(
            jax.ShapeDtypeStruct(residual.shape, F32),
            jax.ShapeDtypeStruct((8,), F32),
            jax.ShapeDtypeStruct((8,), F32),
        ),
        in_specs=[hbm] * 6 + [smem] * 3 + [hbm],
        out_specs=(hbm, smem, smem),
        scratch_shapes=[
            pltpu.VMEM(direction.shape, F32), pltpu.VMEM((32, 256), F32), pltpu.VMEM((256, 256), F32),
            pltpu.VMEM((16, 32), jnp.int32), pltpu.VMEM((256, 256), F32), pltpu.VMEM(direction.shape, F32),
            pltpu.VMEM(direction.shape, F32), dma((6,)), dma,
            pltpu.VMEM((NF, 2, 512, 512), BF),
            pltpu.VMEM((NF, 2, 512, 512), BF),
            pltpu.VMEM((NF, G, G, 2, 32, 128), BF),
            pltpu.VMEM((NF, 2, ROWS, 128), F32), field, field,
            pltpu.VMEM((ROWS, 128), F32), pltpu.VMEM((32, 16, 128), F32),
            pltpu.VMEM((NF, G, G, 2, 32, 128), BF),
            x_part,
            pltpu.VMEM((NF, 2, 32, 128), F32),
            chunks, chunks, chunks, chunks,
            pltpu.VMEM((NF, 2, 2, DEEP, 16, 128), BF), pltpu.VMEM((NF, 2, 2, DEEP, 16, 128), BF),
            pltpu.VMEM((NF, 2, 2, DEEP, 32, 128), BF), pltpu.VMEM((NF, 2, 2, DEEP, 32, 128), BF),
            pltpu.VMEM((NF, 4, 8, 128), F32), pltpu.VMEM((NF, 4, 8, 128), F32),
            pltpu.VMEM((16, 128), F32), pltpu.VMEM((8, 16, 128), F32),
            x_part, x_part, x_part, x_part,
            pltpu.VMEM((8, 128), F32), pltpu.VMEM((16, 8, 128), F32),
            pltpu.VMEM((2, 512, 128), BF),
            dma((NF,)),
            dma((16,)), dma((16,)), dma((16,)), dma((16,)), dma((16,)), dma((16,)),
            dma((NF, 3)), dma((NF, 3)), dma((NF, 3, G)), dma((NF, 3, G)),
            dma((NF, 8)), dma((NF, 8)), dma((8,)), dma((8,)),
            dma((NF, 3, 2)), dma((NF, 3, 2)), dma((NF, G)), dma((NF, G)),
        ],
        compiler_params=pltpu.CompilerParams(
            collective_id=0, has_side_effects=True, vmem_limit_bytes=62 * 1024 * 1024
        ),
        name="hessian_step",
    )(
        direction, noise_weight, jnp.asarray(forward_table), class_map.T, jnp.asarray(back_table), residual,
        class_kappa, step_length, old_norm, spectra.reshape(NF, 2, 512, 512),
    )
    new_residual = residual - delta
    new_norm = jnp.maximum(norm, 0.0)
    new_solution = solution + step_length[:, None, None] * direction
    new_direction = new_residual + growth[:, None, None] * direction
    return (new_solution, new_residual, new_direction, new_norm)


def solution(mesh):
    columns = P("fq", ("sx", "sy"), None)
    return jax.shard_map(
        on_device,
        mesh=mesh,
        in_specs=(
            P("fq", None, "sx", "sy", None), P(("sx", "sy"), None), P("sx", "sy"), P(),
            columns, columns, columns, P("fq"), P("fq"),
        ),
        out_specs=(columns, columns, columns, P("fq")),
        check_vma=False,
    )
```
